128 devices in a mesh: batch: 32 (over y, z, core), mp: 4 (over x).
Axes of the slice: x: 4, y: 4, z: 4, core: 2. Of those that a mesh axis runs over, the one named last changes fastest.
Arguments:
- init_state: float32 [16384, 256], P(('batch', 'mp')), may hold values from -6 to 6
- brownian: bfloat16 [32, 16384, 256], P(None, ('batch', 'mp')), may hold values from -6 to 6
- step_size: float32 [16384], P(('batch', 'mp')), may hold values from 0.02 to 0.1
- lengths: int32 [16384], P(('batch', 'mp')), may hold values from 1 to 32, as said below
- obs_steps: int32 [16384, 8], P(('batch', 'mp')), may hold values from 1 to 32, as said below
- observed: bfloat16 [16384, 8, 128], P(('batch', 'mp')), may hold values from -6 to 6
- w_in: bfloat16 [256, 1024], P(None, 'mp'), may hold values from -0.375 to 0.375
- b_in: bfloat16 [1024], P('mp'), may hold values from -3 to 3
- w_out: bfloat16 [1024, 256], P('mp'), may hold values from -0.1875 to 0.1875
- b_out: float32 [256], replicated, may hold values from -4 to 4
- decoder: bfloat16 [256, 128], replicated, may hold values from -0.375 to 0.375
- prior_rate: float32 [256], replicated, may hold values from 0.1 to 2
- diffusion: float32 [256], replicated, may hold values from 0.7 to 1.4
Outputs:
- elbo_series: float32 [16384], P(('batch', 'mp'))
- scores: float32 [2], replicated
- grad_w_in: float32 [256, 1024], P(None, 'mp')
- grad_b_in: float32 [1024], P('mp')
- grad_w_out: float32 [1024, 256], P('mp')
- grad_b_out: float32 [256], replicated
- grad_decoder: float32 [256, 128], replicated
- grad_init: float32 [16384, 256], P(('batch', 'mp'))
The draws below stay inside these ranges and needn't reach their ends.
Inputs may be any that keep to these rules, and one draw needn't show every extreme that they name: `lengths`: some series has 32 live steps in every draw. obs_steps[i, j] is at most lengths[i].
All inputs are finite; a program needn't handle non-finite values.
Results may differ from the reference program's by a relative error of at most 0.0019.
Values may be sent and summed in bfloat16 or wider, within the bound.
No kernel may reach another device: no remote copies, remote signals or barrier semaphores. Data moves between devices by JAX's collectives and lax.ppermute only.
A program may use at most 64 MiB of HBM per device.

```python
import math
import jax
import jax.numpy as jnp
from jax import lax

L = 256
H = 1024
P_SIZE = 128
OBS = 8
S_STEPS = 32
ROWS_DEV = 128
SERIES = 16384


def length_table(key):
    block_count = SERIES // ROWS_DEV
    key_ceiling, key_choose, key_length, key_place = jax.random.split(jax.random.fold_in(key, 11), 4)
    ceilings = jax.random.randint(key_ceiling, (block_count,), S_STEPS // 4, S_STEPS + 1)
    chosen = jax.random.randint(key_choose, (), 0, block_count)
    ceilings = jnp.where(jnp.arange(block_count) == chosen, S_STEPS, ceilings)
    per_row = jnp.repeat(ceilings, ROWS_DEV, total_repeat_length=SERIES)
    drawn = jax.random.randint(key_length, (SERIES,), 1, per_row + 1)
    places = jax.random.randint(key_place, (block_count,), 0, ROWS_DEV)
    topmost = jnp.arange(SERIES) % ROWS_DEV == jnp.repeat(places, ROWS_DEV, total_repeat_length=SERIES)
    return jnp.where(topmost, per_row, drawn).astype(jnp.int32)


def draw_lengths(key, part):
    return length_table(key)


def draw_obs_steps(key, part):
    table = length_table(key)
    picks = jax.random.randint(jax.random.fold_in(key, 23), (SERIES, OBS), 1, table[:, None] + 1)
    return picks.astype(jnp.int32)


def levels(rng, shape, cuts, smallest, top_value):
    level, own = 1.0, jax.random.fold_in(rng, 6)
    for axis_at, blocks in cuts:
        steps = jnp.exp(jax.random.uniform(jax.random.fold_in(own, axis_at), (blocks,), jnp.float32, smallest / len(cuts), top_value / len(cuts)))
        level = level * jnp.repeat(steps, shape[axis_at] // blocks).reshape([-1 if axis == axis_at else 1 for axis in range(len(shape))])
    return level


def gaussian(own_key, extent, spread, bound, cuts=(), kind=jnp.bfloat16):
    gain = levels(own_key, extent, cuts, -0.22, 0.18) if cuts else 1.0
    values = jax.random.normal(own_key, extent, jnp.float32) * spread * gain
    return jnp.minimum(jnp.maximum(values, -bound), bound).astype(kind)


def setup_inputs(seed: int = 0) -> dict:
    key_list = jax.random.split(jax.random.key(seed), 14)
    init_state = gaussian(key_list[0], (SERIES, L), 1.0, 6.0, ((0, 128),), jnp.float32)
    brownian = gaussian(key_list[1], (S_STEPS, SERIES, L), 1.0, 6.0, ((1, 128),))
    step_size = jnp.clip(jnp.exp(math.log(0.1) - 1.609438 * jax.random.uniform(key_list[2], (SERIES,), jnp.float32) ** levels(key_list[2], (SERIES,), ((0, 128),), -0.2, 0.2)), 0.02, 0.1)
    lengths = draw_lengths(jax.random.fold_in(key_list[13], 71), 0)
    obs_steps = draw_obs_steps(jax.random.fold_in(key_list[13], 71), 0)
    observed = gaussian(key_list[5], (SERIES, OBS, P_SIZE), 1.0, 6.0, ((0, 128),))
    w_in = gaussian(key_list[6], (L, H), L ** -0.5, 0.375, ((1, 4),))
    b_in = gaussian(key_list[7], (H,), 0.5, 3.0, ((0, 4),))
    w_out = gaussian(key_list[8], (H, L), H ** -0.5, 0.1875, ((0, 4),))
    b_out = gaussian(key_list[9], (L,), 1.0, 4.0, (), jnp.float32)
    decoder = gaussian(key_list[10], (L, P_SIZE), L ** -0.5, 0.375)
    prior_rate = jnp.clip(jnp.exp(jax.random.uniform(key_list[11], (L,), jnp.float32, math.log(0.1), math.log(2.0))), 0.1, 2.0)
    diffusion = jnp.clip(jax.random.uniform(key_list[12], (L,), jnp.float32, 0.7, 1.4), 0.7, 1.4)
    return dict(init_state=init_state, brownian=brownian, step_size=step_size, lengths=lengths, obs_steps=obs_steps, observed=observed, w_in=w_in, b_in=b_in, w_out=w_out, b_out=b_out, decoder=decoder, prior_rate=prior_rate, diffusion=diffusion)


def block_terms(block_init, block_noise, block_step, block_lengths, block_obs, block_observed, w_in, b_in, w_out, b_out, decoder, prior_rate, diffusion):
    row_count = block_init.shape[0]
    num_steps = block_noise.shape[0]
    live_mask = (jnp.arange(num_steps, dtype=jnp.int32)[:, None] < block_lengths[None, :]).astype(jnp.float32)
    step_col = block_step[:, None]
    root_col = jnp.sqrt(block_step)[:, None]
    bias_in = b_in.astype(jnp.float32)

    def forward(loop_state, inputs):
        current, kl_sum = loop_state
        increment, live_now = inputs
        activity = jnp.tanh(jnp.dot(current.astype(jnp.bfloat16), w_in, preferred_element_type=jnp.float32) + bias_in).astype(jnp.bfloat16)
        drift_now = jnp.dot(activity, w_out, preferred_element_type=jnp.float32) + b_out
        residual = (drift_now + prior_rate * current) / diffusion
        kl_sum = kl_sum + live_now * 0.5 * block_step * lax.optimization_barrier(jnp.sum(residual * residual, axis=1))
        following = current + live_now[:, None] * (step_col * drift_now + diffusion * root_col * increment.astype(jnp.float32))
        return ((following, kl_sum), (current, activity, residual))
    (last_state, kl_total), (visited, activities, residuals) = lax.scan(forward, (block_init, jnp.zeros((row_count,), jnp.float32)), (block_noise, live_mask))
    trajectory = jnp.concatenate([visited, last_state[None]], axis=0)
    picked = trajectory[block_obs, jnp.arange(row_count, dtype=jnp.int32)[:, None]]
    picked_round = picked.astype(jnp.bfloat16).reshape(-1, picked.shape[2])
    flat_obs = block_observed.reshape(-1, block_observed.shape[2]).astype(jnp.float32)
    misfit = jnp.dot(picked_round, decoder, preferred_element_type=jnp.float32) - flat_obs
    loglik = -0.5 * lax.optimization_barrier(jnp.sum((misfit * misfit).reshape(row_count, -1), axis=1))
    misfit_round = misfit.astype(jnp.bfloat16)
    decoder_grad = jnp.dot(picked_round.T, misfit_round, preferred_element_type=jnp.float32)
    misfit_back = jnp.dot(misfit_round, decoder.T, preferred_element_type=jnp.float32).reshape(row_count, block_obs.shape[1], -1)
    onehot = (block_obs[:, :, None] == jnp.arange(num_steps + 1, dtype=jnp.int32)[None, None, :]).astype(jnp.float32)
    obs_back = jnp.einsum('bjs,bjl->sbl', onehot, misfit_back, precision=lax.Precision.HIGHEST)

    def backward(loop_state, inputs):
        cotangent, sum_w_in, sum_b_in, sum_w_out, sum_b_out = loop_state
        current, activity, residual, live_now, obs_here = inputs
        factor = (live_now * block_step)[:, None]
        scaled = residual / diffusion
        update = factor * (cotangent + scaled)
        update_round = update.astype(jnp.bfloat16)
        activity_value = activity.astype(jnp.float32)
        pre_grad = jnp.dot(update_round, w_out.T, preferred_element_type=jnp.float32) * (1.0 - activity_value * activity_value)
        pre_round = pre_grad.astype(jnp.bfloat16)
        cotangent = cotangent + factor * prior_rate * scaled + jnp.dot(pre_round, w_in.T, preferred_element_type=jnp.float32) + obs_here
        sum_w_in = sum_w_in + jnp.dot(current.astype(jnp.bfloat16).T, pre_round, preferred_element_type=jnp.float32)
        sum_b_in = sum_b_in + lax.optimization_barrier(jnp.sum(pre_grad, axis=0))
        sum_w_out = sum_w_out + jnp.dot(activity.T, update_round, preferred_element_type=jnp.float32)
        sum_b_out = sum_b_out + lax.optimization_barrier(jnp.sum(update, axis=0))
        return ((cotangent, sum_w_in, sum_b_in, sum_w_out, sum_b_out), None)
    start_back = (obs_back[num_steps], jnp.zeros(w_in.shape, jnp.float32), jnp.zeros((w_in.shape[1],), jnp.float32), jnp.zeros(w_out.shape, jnp.float32), jnp.zeros((w_out.shape[1],), jnp.float32))
    (cotangent, sum_w_in, sum_b_in, sum_w_out, sum_b_out), _ = lax.scan(backward, start_back, (visited, activities, residuals, live_mask, obs_back[:num_steps]), reverse=True)
    divisor = (L * block_lengths + P_SIZE * OBS).astype(jnp.float32)
    elbo_rows = (loglik - kl_total) / divisor
    return (elbo_rows, cotangent, jnp.sum(loglik), jnp.sum(kl_total), sum_w_in, sum_b_in, sum_w_out, sum_b_out, decoder_grad)

def reference(init_state, brownian, step_size, lengths, obs_steps, observed, w_in, b_in, w_out, b_out, decoder, prior_rate, diffusion):
    block_count = SERIES // ROWS_DEV
    blocked = (init_state.reshape(block_count, ROWS_DEV, L), jnp.transpose(brownian.reshape(S_STEPS, block_count, ROWS_DEV, L), (1, 0, 2, 3)), step_size.reshape(block_count, ROWS_DEV), lengths.reshape(block_count, ROWS_DEV), obs_steps.reshape(block_count, ROWS_DEV, OBS), observed.reshape(block_count, ROWS_DEV, OBS, P_SIZE))
    zero_totals = (jnp.zeros((L, H), jnp.float32), jnp.zeros((H,), jnp.float32), jnp.zeros((H, L), jnp.float32), jnp.zeros((L,), jnp.float32), jnp.zeros((L, P_SIZE), jnp.float32), jnp.zeros((), jnp.float32), jnp.zeros((), jnp.float32))

    def visit(totals, pieces):
        outcome = block_terms(pieces[0], pieces[1], pieces[2], pieces[3], pieces[4], pieces[5], w_in, b_in, w_out, b_out, decoder, prior_rate, diffusion)
        elbo_rows, init_grad, loglik_sum, kl_sum, sum_w_in, sum_b_in, sum_w_out, sum_b_out, decoder_grad = outcome
        fresh = (sum_w_in, sum_b_in, sum_w_out, sum_b_out, decoder_grad, loglik_sum, kl_sum)
        totals = tuple((first + second for first, second in zip(totals, fresh)))
        return (totals, (elbo_rows, init_grad))
    totals, (elbo_rows, init_grads) = lax.scan(visit, zero_totals, blocked)
    elbo_series = elbo_rows.reshape(SERIES)
    grad_init = init_grads.reshape(SERIES, L)
    scores = jnp.stack([totals[5] / SERIES, totals[6] / SERIES])
    return (elbo_series, scores, totals[0] / SERIES, totals[1] / SERIES, totals[2] / SERIES, totals[3] / SERIES, totals[4] / SERIES, grad_init)
```

```python
import functools

import jax
import jax.numpy as jnp
from jax import lax
from jax.experimental import pallas as pl
from jax.experimental.pallas import tpu as pltpu

F32 = jnp.float32
BF16 = jnp.bfloat16


def wide(x):
    return jnp.concatenate([x, x], axis=1)


def column(row, rows):
    return jnp.transpose(jnp.broadcast_to(row, (rows, rows)))


def series_kernel(
    init,
    brown,
    step,
    lens,
    obs_steps,
    obs,
    w_in,
    b_in,
    w_out,
    b_out,
    dec,
    prior,
    diff,
    grads,
    dec_grad,
    in_bias,
    out_bias,
    sums,
    elbo,
    grad_init,
    act,
    pg,
    low,
    upd,
    scaled,
    w_in_t,
    w_out_t,
    obs_at,
    state,
    kl_acc,
    sq_acc,
    in_acc,
    out_acc,
    acc_in,
    acc_out,
):
    steps, rows, width = brown.shape
    parts = w_in.shape[0]
    share = w_in.shape[2]
    hidden = parts * share
    cols = dec.shape[1]
    seen = obs.shape[0]

    step_b = column(step[...], rows)
    root_b = jnp.sqrt(step_b)
    lens_b = column(lens[...], rows)
    inv = 1.0 / diff[...]
    for j in range(seen):
        obs_at[j] = jnp.broadcast_to(obs_steps[:, j : j + 1], (rows, cols))
    for q in range(parts):
        w_out_t[q] = jnp.transpose(w_out[q])
        w_in_t[q * share : (q + 1) * share, :] = jnp.transpose(w_in[q])
    dec_t = jnp.transpose(dec[...])
    w_in_t[hidden : hidden + cols, :] = dec_t
    w_in_t[hidden + cols : hidden + 2 * cols, :] = dec_t

    state[...] = init[...]
    kl_acc[...] = jnp.zeros_like(kl_acc)
    sq_acc[...] = jnp.zeros_like(sq_acc)
    in_acc[...] = jnp.zeros_like(in_acc)
    out_acc[...] = jnp.zeros_like(out_acc)
    acc_in[...] = jnp.zeros_like(acc_in)
    acc_out[...] = jnp.zeros_like(acc_out)

    def observe(k, low_now):
        seen_now = jnp.dot(low_now, dec[...], preferred_element_type=F32)
        total = jnp.zeros((rows, cols), F32)
        squares = sq_acc[...]
        for j in range(seen):
            misfit = jnp.where(obs_at[j] == k, seen_now - obs[j].astype(F32), 0.0)
            squares = squares + misfit * misfit
            total = total + misfit.astype(BF16).astype(F32)
        sq_acc[...] = squares
        high = total.astype(BF16)
        pg[k, :, hidden : hidden + cols] = high
        pg[k, :, hidden + cols : hidden + 2 * cols] = (total - high.astype(F32)).astype(BF16)

    def forward(k, _):
        now = state[...]
        low_now = now.astype(BF16)
        low[k] = low_now
        for q in range(parts):
            block = slice(q * share, (q + 1) * share)
            pre = jnp.dot(low_now, w_in[q], preferred_element_type=F32) + b_in[:, block]
            act[k, :, block] = jnp.tanh(pre).astype(BF16)
        observe(k, low_now)
        drift = (
            jnp.dot(act[k], w_out[...].reshape(hidden, width), preferred_element_type=F32)
            + b_out[...]
        )
        live = k < lens_b
        factor = wide(jnp.where(live, step_b, 0.0))
        noise = wide(jnp.where(live, root_b, 0.0))
        residual = (drift + prior[...] * now) * inv
        scaled[k] = residual * inv
        spent = factor * (residual * residual)
        kl_acc[...] += spent[:, :rows] + spent[:, rows:]
        state[...] = now + (factor * drift + diff[...] * noise * brown[k].astype(F32))
        return 0

    lax.fori_loop(0, steps, forward, 0)
    last = state[...].astype(BF16)
    low[steps] = last
    observe(steps, last)

    state[...] = jnp.dot(
        pg[steps, :, hidden:], w_in_t[hidden:, :], preferred_element_type=F32
    )

    def backward(i, _):
        k = steps - 1 - i
        cot = state[...]
        factor = wide(jnp.where(k < lens_b, step_b, 0.0))
        pull = scaled[k]
        update = factor * (cot + pull)
        low_up = update.astype(BF16)
        upd[k] = low_up
        out_acc[...] += jnp.sum(update.reshape(rows // 8, 8, width), axis=0)
        for q in range(parts):
            block = slice(q * share, (q + 1) * share)
            a = act[k, :, block].astype(F32)
            pre = jnp.dot(low_up, w_out_t[q], preferred_element_type=F32) * (1.0 - a * a)
            pg[k, :, block] = pre.astype(BF16)
            in_acc[:, block] += jnp.sum(pre.reshape(rows // 8, 8, share), axis=0)
        state[...] = (
            cot
            + factor * (prior[...] * pull)
            + jnp.dot(pg[k], w_in_t[...], preferred_element_type=F32)
        )
        return 0

    lax.fori_loop(0, steps, backward, 0)
    grad_init[...] = state[...]

    chunk = 4
    turned = (((0,), (0,)), ((), ()))

    def gather_grads(i, _):
        at = pl.ds(i * chunk, chunk)
        acc_in[...] += lax.dot_general(
            low[at].reshape(chunk * rows, width),
            pg[at].reshape(chunk * rows, hidden + 2 * cols),
            turned,
            preferred_element_type=F32,
        )
        acc_out[...] += lax.dot_general(
            upd[at].reshape(chunk * rows, width),
            act[at].reshape(chunk * rows, hidden),
            turned,
            preferred_element_type=F32,
        )
        return 0

    lax.fori_loop(0, steps // chunk, gather_grads, 0)
    final = acc_in[:, hidden:] + lax.dot_general(
        low[steps], pg[steps, :, hidden:], turned, preferred_element_type=F32
    )
    dec_grad[...] = final[:, :cols] + final[:, cols:]
    for q in range(parts):
        block = slice(q * share, (q + 1) * share)
        grads[q, :width, :] = acc_in[:, block]
        grads[q, width:, :] = acc_out[:, block]
    in_bias[...] = jnp.sum(in_acc[...], axis=0, keepdims=True)
    out_bias[...] = jnp.sum(out_acc[...], axis=0, keepdims=True)

    kl = 0.5 * jnp.sum(jnp.transpose(kl_acc[...]), axis=0, keepdims=True)
    loglik = -0.5 * jnp.sum(jnp.transpose(sq_acc[...]), axis=0, keepdims=True)
    sums[0:1, :] = loglik
    sums[1:2, :] = kl
    divisor = (width * lens[...] + cols * seen).astype(F32)
    elbo[...] = (loglik - kl) / divisor


def solve(init, brown, step, lengths, obs_steps, observed, w_in, b_in, w_out, b_out, dec, prior, diff):
    rows, width = init.shape
    steps = brown.shape[0]
    parts, _, share = w_in.shape
    hidden = parts * share
    seen, cols = observed.shape[1:]
    vmem = pl.BlockSpec(memory_space=pltpu.VMEM)
    shape = jax.ShapeDtypeStruct
    outs = (
        shape((parts, 2 * width, share), F32),
        shape((width, cols), F32),
        shape((1, hidden), F32),
        shape((1, width), F32),
        shape((2, rows), F32),
        shape((1, rows), F32),
        shape((rows, width), F32),
    )
    return pl.pallas_call(
        series_kernel,
        name="series",
        out_shape=outs,
        in_specs=[vmem] * 13,
        out_specs=(vmem,) * len(outs),
        scratch_shapes=[
            pltpu.VMEM((steps, rows, hidden), BF16),
            pltpu.VMEM((steps + 1, rows, hidden + 2 * cols), BF16),
            pltpu.VMEM((steps + 1, rows, width), BF16),
            pltpu.VMEM((steps, rows, width), BF16),
            pltpu.VMEM((steps, rows, width), F32),
            pltpu.VMEM((hidden + 2 * cols, width), BF16),
            pltpu.VMEM((parts, width, share), BF16),
            pltpu.VMEM((seen, rows, cols), jnp.int32),
            pltpu.VMEM((rows, width), F32),
            pltpu.VMEM((rows, rows), F32),
            pltpu.VMEM((rows, cols), F32),
            pltpu.VMEM((8, hidden), F32),
            pltpu.VMEM((8, width), F32),
            pltpu.VMEM((width, hidden + 2 * cols), F32),
            pltpu.VMEM((width, hidden), F32),
        ],
        compiler_params=pltpu.CompilerParams(vmem_limit_bytes=60 * 1024 * 1024),
        cost_estimate=pl.CostEstimate(
            flops=12 * steps * rows * width * hidden,
            bytes_accessed=8 * 1024 * 1024,
            transcendentals=steps * rows * hidden,
        ),
    )(
        init,
        brown,
        step[None],
        lengths[None],
        obs_steps,
        jnp.transpose(observed, (1, 0, 2)),
        w_in,
        b_in,
        w_out,
        b_out[None],
        dec,
        prior[None],
        diff[None],
    )


AXES = ("batch", "mp")


def on_device(
    init_state,
    brownian,
    step_size,
    lengths,
    obs_steps,
    observed,
    w_in,
    b_in,
    w_out,
    b_out,
    decoder,
    prior_rate,
    diffusion,
):
    w_in_all = lax.all_gather(w_in, "mp", axis=0)
    w_out_all = lax.all_gather(w_out, "mp", axis=0)
    b_in_all = lax.all_gather(b_in, "mp", axis=0, tiled=True).astype(F32)[None]
    grads, dec_grad, in_bias, out_bias, sums, elbo, grad_init = solve(
        init_state,
        brownian,
        step_size,
        lengths,
        obs_steps,
        observed,
        w_in_all,
        b_in_all,
        w_out_all,
        b_out,
        decoder,
        prior_rate,
        diffusion,
    )
    total = init_state.shape[0] * lax.axis_size("batch") * lax.axis_size("mp")
    width = init_state.shape[1]
    share = w_in.shape[1]
    hidden = share * lax.axis_size("mp")
    own = lax.psum_scatter(grads, "mp", scatter_dimension=0)
    own = lax.psum(own, "batch") / total
    flat = jnp.concatenate(
        [dec_grad.reshape(-1), in_bias.reshape(-1), out_bias.reshape(-1), jnp.sum(sums, axis=1)]
    )
    flat = lax.psum(flat, AXES) / total
    size = dec_grad.size
    all_in_bias = flat[size : size + hidden]
    own_in_bias = lax.dynamic_slice_in_dim(all_in_bias, lax.axis_index("mp") * share, share, 0)
    return (
        elbo.reshape(-1),
        flat[size + hidden + width :],
        own[:width],
        own_in_bias,
        own[width:].T,
        flat[size + hidden : size + hidden + width],
        flat[:size].reshape(dec_grad.shape),
        grad_init,
    )


def solution(mesh):
    from jax.sharding import PartitionSpec as P

    return jax.shard_map(
        on_device,
        mesh=mesh,
        in_specs=(
            P(AXES, None),
            P(None, AXES, None),
            P(AXES),
            P(AXES),
            P(AXES, None),
            P(AXES, None, None),
            P(None, "mp"),
            P("mp"),
            P("mp", None),
            P(),
            P(),
            P(),
            P(),
        ),
        out_specs=(
            P(AXES),
            P(),
            P(None, "mp"),
            P("mp"),
            P("mp", None),
            P(),
            P(),
            P(AXES, None),
        ),
        check_vma=False,
    )
```

```python
import functools

import jax
import jax.numpy as jnp
from jax import lax
from jax.experimental import pallas as pl
from jax.experimental.pallas import tpu as pltpu
from jax.sharding import Mesh
from jax.sharding import PartitionSpec as P

F32 = jnp.float32
BF16 = jnp.bfloat16


def wide(x):
    return jnp.concatenate([x, x], axis=1)


def column(row, rows):
    return jnp.transpose(jnp.broadcast_to(row, (rows, rows)))


def series_kernel(
    init,
    brown,
    step,
    lens,
    obs_steps,
    obs,
    piece_0,
    piece_1,
    piece_2,
    piece_3,
    b_out,
    dec,
    prior,
    diff,
    place,
    keep,
    send,
    elbo,
    grad_init,
    act,
    pg,
    low,
    upd,
    scaled,
    b_in,
    w_out,
    w_in_t,
    w_out_t,
    obs_at,
    state,
    kl_acc,
    sq_acc,
    in_acc,
    out_acc,
    acc,
    acc_dec,
):
    steps, rows, width = brown.shape
    pieces = (piece_0, piece_1, piece_2, piece_3)
    parts = len(pieces)
    share = piece_0.shape[1]
    hidden = parts * share
    cols = dec.shape[1]
    seen = obs.shape[0]

    step_b = column(step[...], rows)
    root_b = jnp.sqrt(step_b)
    lens_b = column(lens[...], rows)
    inv = 1.0 / diff[...]
    for j in range(seen):
        obs_at[j] = column(obs_steps[j : j + 1, :], rows)
    for q, piece in enumerate(pieces):
        block = slice(q * share, (q + 1) * share)
        w_out[block, :] = piece[width : width + share, :]
        w_out_t[q] = jnp.transpose(piece[width : width + share, :])
        w_in_t[block, :] = jnp.transpose(piece[:width, :])
        b_in[:, block] = piece[width + share :, :].astype(F32)[:1]
    dec_t = jnp.transpose(dec[...])
    w_in_t[hidden : hidden + cols, :] = dec_t
    w_in_t[hidden + cols : hidden + 2 * cols, :] = dec_t

    state[...] = init[...]
    kl_acc[...] = jnp.zeros_like(kl_acc)
    sq_acc[...] = jnp.zeros_like(sq_acc)
    in_acc[...] = jnp.zeros_like(in_acc)
    out_acc[...] = jnp.zeros_like(out_acc)
    acc[...] = jnp.zeros_like(acc)
    acc_dec[...] = jnp.zeros_like(acc_dec)

    def observe(k, low_now):
        seen_now = jnp.dot(low_now, dec[...], preferred_element_type=F32)
        total = jnp.zeros((rows, cols), F32)
        squares = sq_acc[...]
        for j in range(seen):
            misfit = jnp.where(obs_at[j] == k, seen_now - obs[j].astype(F32), 0.0)
            squares = squares + misfit * misfit
            total = total + misfit.astype(BF16).astype(F32)
        sq_acc[...] = squares
        high = total.astype(BF16)
        pg[k, :, hidden : hidden + cols] = high
        pg[k, :, hidden + cols : hidden + 2 * cols] = (total - high.astype(F32)).astype(BF16)

    def forward(k, _):
        now = state[...]
        low_now = now.astype(BF16)
        low[k] = low_now
        for q in range(parts):
            block = slice(q * share, (q + 1) * share)
            pre = jnp.dot(low_now, pieces[q][:width, :], preferred_element_type=F32) + b_in[:, block]
            act[k, :, block] = jnp.tanh(pre).astype(BF16)
        observe(k, low_now)
        drift = (
            jnp.dot(act[k], w_out[...], preferred_element_type=F32)
            + b_out[...]
        )
        live = k < lens_b
        factor = wide(jnp.where(live, step_b, 0.0))
        noise = wide(jnp.where(live, root_b, 0.0))
        residual = (drift + prior[...] * now) * inv
        scaled[k] = residual * inv
        spent = factor * (residual * residual)
        kl_acc[...] += spent[:, :rows] + spent[:, rows:]
        state[...] = now + (factor * drift + diff[...] * noise * brown[k].astype(F32))
        return 0

    lax.fori_loop(0, steps, forward, 0)
    last = state[...].astype(BF16)
    low[steps] = last
    observe(steps, last)

    state[...] = jnp.dot(
        pg[steps, :, hidden:], w_in_t[hidden:, :], preferred_element_type=F32
    )

    def backward(i, _):
        k = steps - 1 - i
        cot = state[...]
        factor = wide(jnp.where(k < lens_b, step_b, 0.0))
        pull = scaled[k]
        update = factor * (cot + pull)
        low_up = update.astype(BF16)
        upd[k] = low_up
        out_acc[...] += jnp.sum(update.reshape(rows // 8, 8, width), axis=0)
        for q in range(parts):
            block = slice(q * share, (q + 1) * share)
            a = act[k, :, block].astype(F32)
            pre = jnp.dot(low_up, w_out_t[q], preferred_element_type=F32) * (1.0 - a * a)
            pg[k, :, block] = pre.astype(BF16)
            in_acc[:, block] += jnp.sum(pre.reshape(rows // 8, 8, share), axis=0)
        state[...] = (
            cot
            + factor * (prior[...] * pull)
            + jnp.dot(pg[k], w_in_t[...], preferred_element_type=F32)
        )
        return 0

    lax.fori_loop(0, steps, backward, 0)
    grad_init[...] = state[...]

    chunk = 4
    turned = (((0,), (0,)), ((), ()))

    def gather_grads(i, _):
        at = pl.ds(i * chunk, chunk)
        left = low[at].reshape(chunk * rows, width)
        right = pg[at].reshape(chunk * rows, hidden + 2 * cols)
        acc[0] += lax.dot_general(left, right[:, :hidden], turned, preferred_element_type=F32)
        acc_dec[...] += lax.dot_general(
            left, right[:, hidden:], turned, preferred_element_type=F32
        )
        acc[1] += lax.dot_general(
            upd[at].reshape(chunk * rows, width),
            act[at].reshape(chunk * rows, hidden),
            turned,
            preferred_element_type=F32,
        )
        return 0

    lax.fori_loop(0, steps // chunk, gather_grads, 0)
    final = acc_dec[...] + lax.dot_general(
        low[steps], pg[steps, :, hidden:], turned, preferred_element_type=F32
    )
    core = place[0]
    spot = place[1]
    slots = keep.shape[0]
    deep = width // slots
    halves = share // cols
    acc_dec[:, :cols] = final[:, :cols] + final[:, cols:]
    in_sum = jnp.sum(in_acc[...], axis=0, keepdims=True)
    out_sum = jnp.sum(out_acc[...], axis=0, keepdims=True)
    kl = 0.5 * jnp.sum(jnp.transpose(kl_acc[...]), axis=0, keepdims=True)
    loglik = -0.5 * jnp.sum(jnp.transpose(sq_acc[...]), axis=0, keepdims=True)
    rest = [out_sum[:, p * cols : (p + 1) * cols] for p in range(width // cols)]
    rest = rest + [loglik, kl]
    rest = rest + [jnp.zeros((8 - halves - len(rest), cols), F32)]
    base = halves * deep
    tile = slots * 8
    for half, out in ((core, keep), (1 - core, send)):
        decs = acc_dec[pl.ds(pl.multiple_of(half * tile, 8), tile), :cols].reshape(slots, 8, cols)
        for s in range(parts):
            q = lax.rem(spot + (parts - s), parts)
            aux = [in_sum[:, s * share + p * cols : s * share + (p + 1) * cols] for p in range(halves)]
            aux = jnp.concatenate(aux + rest, axis=0)
            for p in range(halves):
                block = slice(s * share + p * cols, s * share + (p + 1) * cols)
                out[:, q, p * deep : (p + 1) * deep, :] = acc[half, :, block].reshape(
                    slots, deep, cols
                )
            out[:, q, base : base + 8, :] = decs
            out[:, q, base + 8 : base + 16, :] = jnp.broadcast_to(aux[None], (slots, 8, cols))
    divisor = (width * lens[...] + cols * seen).astype(F32)
    elbo[...] = (loglik - kl) / divisor


def solve(init, brown, step, lengths, obs_steps, observed, pieces, b_out, dec, prior, diff, place, slots):
    rows, width = init.shape
    steps = brown.shape[0]
    parts = len(pieces)
    share = pieces[0].shape[1]
    hidden = parts * share
    seen, cols = observed.shape[1:]
    vmem = pl.BlockSpec(memory_space=pltpu.VMEM)
    shape = jax.ShapeDtypeStruct
    payload = shape((slots, parts, width // slots * share // cols + 16, cols), F32)
    outs = (
        payload,
        payload,
        shape((1, rows), F32),
        shape((rows, width), F32),
    )
    return pl.pallas_call(
        series_kernel,
        name="series",
        out_shape=outs,
        in_specs=[vmem] * (10 + parts) + [pl.BlockSpec(memory_space=pltpu.SMEM)],
        out_specs=(vmem,) * len(outs),
        scratch_shapes=[
            pltpu.VMEM((steps, rows, hidden), BF16),
            pltpu.VMEM((steps + 1, rows, hidden + 2 * cols), BF16),
            pltpu.VMEM((steps + 1, rows, width), BF16),
            pltpu.VMEM((steps, rows, width), BF16),
            pltpu.VMEM((steps, rows, width), F32),
            pltpu.VMEM((1, hidden), F32),
            pltpu.VMEM((hidden, width), BF16),
            pltpu.VMEM((hidden + 2 * cols, width), BF16),
            pltpu.VMEM((parts, width, share), BF16),
            pltpu.VMEM((seen, rows, cols), jnp.int32),
            pltpu.VMEM((rows, width), F32),
            pltpu.VMEM((rows, rows), F32),
            pltpu.VMEM((rows, cols), F32),
            pltpu.VMEM((8, hidden), F32),
            pltpu.VMEM((8, width), F32),
            pltpu.VMEM((2, width, hidden), F32),
            pltpu.VMEM((width, 2 * cols), F32),
        ],
        compiler_params=pltpu.CompilerParams(vmem_limit_bytes=48 * 1024 * 1024),
        cost_estimate=pl.CostEstimate(
            flops=12 * steps * rows * width * hidden,
            bytes_accessed=8 * 1024 * 1024,
            transcendentals=steps * rows * hidden,
        ),
    )(
        init,
        brown,
        step[None],
        lengths[None],
        obs_steps.T,
        jnp.transpose(observed, (1, 0, 2)),
        *pieces,
        b_out[None],
        dec,
        prior[None],
        diff[None],
        place,
    )


def sum_kernel(scale, parts, spread, rest):
    depth = spread.shape[1]
    total = jnp.sum(parts[...], axis=0) * scale
    spread[...] = jnp.broadcast_to(total[None, :depth], spread.shape)
    rest[...] = total[depth:]


def sum_parts(parts, slots, scale):
    _, depth, cols = parts.shape
    vmem = pl.BlockSpec(memory_space=pltpu.VMEM)
    return pl.pallas_call(
        functools.partial(sum_kernel, scale),
        name="sum_parts",
        out_shape=(
            jax.ShapeDtypeStruct((slots, depth - 8, cols), F32),
            jax.ShapeDtypeStruct((8, cols), F32),
        ),
        in_specs=[vmem],
        out_specs=(vmem, vmem),
        compiler_params=pltpu.CompilerParams(vmem_limit_bytes=8 * 1024 * 1024),
    )(parts)


def lay_kernel(place, mine, other, w_in, w_out, dec):
    core = place[0]
    slots, depth, cols = mine.shape
    width = w_in.shape[0]
    deep = width // slots

    def lay(low, high):
        for p in range(w_in.shape[1] // cols):
            rows = slice(p * deep, (p + 1) * deep)
            block = slice(p * cols, (p + 1) * cols)
            w_in[:, block] = low[:, rows, :].reshape(width, cols)
            w_out[block, :] = jnp.transpose(high[:, rows, :].reshape(width, cols))
        dec[: slots * 8, :] = low[:, depth - 8 :, :].reshape(slots * 8, cols)
        dec[slots * 8 :, :] = high[:, depth - 8 :, :].reshape(slots * 8, cols)

    pl.when(core == 0)(lambda: lay(mine, other))
    pl.when(core == 1)(lambda: lay(other, mine))


def lay_out(place, mine, other, width, share, cols):
    vmem = pl.BlockSpec(memory_space=pltpu.VMEM)
    shape = jax.ShapeDtypeStruct
    return pl.pallas_call(
        lay_kernel,
        name="lay_out",
        out_shape=(
            shape((width, share), F32),
            shape((share, width), F32),
            shape((width, cols), F32),
        ),
        in_specs=[pl.BlockSpec(memory_space=pltpu.SMEM), vmem, vmem],
        out_specs=(vmem,) * 3,
        compiler_params=pltpu.CompilerParams(vmem_limit_bytes=8 * 1024 * 1024),
    )(place, mine, other)


AXES = ("y", "z", "c", "x")
RING = ("y", "z", "x")


def shifted(array, axis, by):
    count = lax.axis_size(axis)
    return lax.ppermute(array, axis, [(i, (i + by) % count) for i in range(count)])


def on_device(
    init_state,
    brownian,
    step_size,
    lengths,
    obs_steps,
    observed,
    w_in,
    b_in,
    w_out,
    b_out,
    decoder,
    prior_rate,
    diffusion,
):
    width = init_state.shape[1]
    share = w_in.shape[1]
    parts = lax.axis_size("x")
    slots = lax.axis_size("y") * lax.axis_size("z")
    cols = decoder.shape[1]
    core = lax.axis_index("c")
    spot = lax.axis_index("x")

    mine = jnp.concatenate([w_in, w_out, jnp.broadcast_to(b_in[None], (16, share))], axis=0)
    pieces = [mine] + [shifted(mine, "x", by) for by in range(1, parts)]
    place = jnp.stack([core, spot]).astype(jnp.int32)
    keep, send, elbo, grad_init = solve(
        init_state,
        brownian,
        step_size,
        lengths,
        obs_steps,
        observed,
        pieces,
        b_out,
        decoder,
        prior_rate,
        diffusion,
        place,
        slots,
    )
    scale = 1.0 / (init_state.shape[0] * lax.axis_size(AXES))
    chip = keep + shifted(send, "c", 1)
    members = slots * parts
    received = lax.all_to_all(chip.reshape(members, -1, cols), RING, 0, 0, tiled=True)
    spread, rest = sum_parts(received, slots, scale)
    own = lax.all_to_all(spread, ("y", "z"), 0, 0, tiled=True)
    other = shifted(own, "c", 1)
    grad_w_in, grad_w_out, grad_decoder = lay_out(place, own, other, width, share, cols)
    per = share // cols
    end = per + width // cols
    return (
        elbo.reshape(-1),
        jnp.sum(rest[end : end + 2], axis=1),
        grad_w_in,
        rest[:per].reshape(-1),
        grad_w_out,
        rest[per:end].reshape(-1),
        grad_decoder,
        grad_init,
    )


def solution(mesh):
    torus = Mesh(mesh.devices.reshape(4, 4, 2, mesh.shape["mp"]), AXES)
    return jax.shard_map(
        on_device,
        mesh=torus,
        in_specs=(
            P(AXES, None),
            P(None, AXES, None),
            P(AXES),
            P(AXES),
            P(AXES, None),
            P(AXES, None, None),
            P(None, "x"),
            P("x"),
            P("x", None),
            P(),
            P(),
            P(),
            P(),
        ),
        out_specs=(
            P(AXES),
            P(),
            P(None, "x"),
            P("x"),
            P("x", None),
            P(),
            P(),
            P(AXES, None),
        ),
        check_vma=False,
    )
```

```python
import functools

import jax
import jax.numpy as jnp
from jax import lax
from jax.experimental import pallas as pl
from jax.experimental.pallas import tpu as pltpu
from jax.sharding import Mesh
from jax.sharding import PartitionSpec as P

F32 = jnp.float32
BF16 = jnp.bfloat16


def wide(x):
    return jnp.concatenate([x, x], axis=1)


def column(row, rows):
    return jnp.transpose(jnp.broadcast_to(row, (rows, rows)))


def series_kernel(
    brown_home,
    packed,
    obs,
    piece_0,
    piece_1,
    piece_2,
    piece_3,
    place,
    keep,
    send,
    elbo,
    grad_init,
    act,
    seen_back,
    low,
    pg_a,
    pg_b,
    upd_a,
    upd_b,
    scaled,
    b_in,
    w_out,
    w_in_t,
    w_out_t,
    obs_at,
    state,
    kl_acc,
    sq_acc,
    in_acc,
    out_acc,
    acc,
    acc_dec,
    brown,
    dec,
    done,
):
    fetch = pltpu.make_async_copy(brown_home, brown, done)
    fetch.start()
    steps, rows, width = brown.shape
    pieces = (piece_0, piece_1, piece_2, piece_3)
    parts = len(pieces)
    share = piece_0.shape[1]
    hidden = parts * share
    cols = dec.shape[1]
    seen = obs.shape[0]
    first, last_row = packed[:rows, :], packed[rows : rows + 8, :]
    b_out, prior, diff = last_row[0:1], last_row[1:2], last_row[2:3]
    step, lens = last_row[3:4, :rows], last_row[3:4, rows:]
    dec_home = packed[rows + 8 :, :].astype(BF16)
    dec[:rows, :] = dec_home[:, :cols]
    dec[rows:, :] = dec_home[:, cols:]

    for q, piece in enumerate(pieces):
        block = slice(q * share, (q + 1) * share)
        w_out[block, :] = piece[width : width + share, :]
        w_out_t[q] = jnp.transpose(piece[width : width + share, :])
        w_in_t[block, :] = jnp.transpose(piece[:width, :])
        b_in[:, block] = piece[width + share :, :].astype(F32)[:1]
    step_b = column(step, rows)
    root_b = jnp.sqrt(step_b)
    lens_b = column(lens, rows)
    inv = 1.0 / diff
    for j in range(seen):
        half = (j % 2) * rows
        obs_at[j] = column(last_row[4 + j // 2 : 5 + j // 2, half : half + rows], rows)
    dec_t = jnp.transpose(dec[...])
    w_in_t[hidden : hidden + cols, :] = dec_t
    w_in_t[hidden + cols : hidden + 2 * cols, :] = dec_t

    state[...] = first
    kl_acc[...] = jnp.zeros_like(kl_acc)
    sq_acc[...] = jnp.zeros_like(sq_acc)
    in_acc[...] = jnp.zeros_like(in_acc)
    out_acc[...] = jnp.zeros_like(out_acc)
    acc[...] = jnp.zeros_like(acc)
    acc_dec[...] = jnp.zeros_like(acc_dec)

    def observe(k, low_now):
        k_now = jnp.asarray(k, jnp.int32).astype(F32)
        seen_now = jnp.dot(low_now, dec[...], preferred_element_type=F32)
        total = jnp.zeros((rows, cols), F32)
        squares = sq_acc[...]
        for j in range(seen):
            misfit = jnp.where(obs_at[j] == k_now, seen_now - obs[j].astype(F32), 0.0)
            squares = squares + misfit * misfit
            total = total + misfit.astype(BF16).astype(F32)
        sq_acc[...] = squares
        high = total.astype(BF16)
        seen_back[k, :, :cols] = high
        seen_back[k, :, cols:] = (total - high.astype(F32)).astype(BF16)

    def forward(k, _):
        now = state[...]
        low_now = now.astype(BF16)
        low[k] = low_now
        for q in range(parts):
            block = slice(q * share, (q + 1) * share)
            pre = jnp.dot(low_now, pieces[q][:width, :], preferred_element_type=F32) + b_in[:, block]
            act[k, :, block] = jnp.tanh(pre).astype(BF16)
        observe(k, low_now)
        drift = (
            jnp.dot(act[k], w_out[...], preferred_element_type=F32)
            + b_out
        )
        live = k.astype(F32) < lens_b
        factor = wide(jnp.where(live, step_b, 0.0))
        noise = wide(jnp.where(live, root_b, 0.0))
        residual = (drift + prior * now) * inv
        scaled[k] = residual * inv
        spent = factor * (residual * residual)
        kl_acc[...] += spent[:, :rows] + spent[:, rows:]
        state[...] = now + (factor * drift + diff * noise * brown[k].astype(F32))
        return 0

    fetch.wait()
    lax.fori_loop(0, steps, forward, 0)
    last = state[...].astype(BF16)
    low[steps] = last
    observe(steps, last)

    state[...] = jnp.dot(
        seen_back[steps], w_in_t[hidden:, :], preferred_element_type=F32
    )

    turned = (((0,), (0,)), ((), ()))

    def back_pair(k_low, pg_now, upd_now):
        for slot in (1, 0):
            k = k_low + slot
            cot = state[...]
            factor = wide(jnp.where(k.astype(F32) < lens_b, step_b, 0.0))
            pull = scaled[k]
            update = factor * (cot + pull)
            low_up = update.astype(BF16)
            upd_now[slot] = low_up
            out_acc[...] += jnp.sum(update.reshape(rows // 8, 8, width), axis=0)
            for q in range(parts):
                block = slice(q * share, (q + 1) * share)
                a = act[k, :, block].astype(F32)
                pre = jnp.dot(low_up, w_out_t[q], preferred_element_type=F32) * (1.0 - a * a)
                pg_now[slot, :, block] = pre.astype(BF16)
                in_acc[:, block] += jnp.sum(pre.reshape(rows // 8, 8, share), axis=0)
            pg_now[slot, :, hidden:] = seen_back[k]
            state[...] = (
                cot
                + factor * (prior * pull)
                + jnp.dot(pg_now[slot], w_in_t[...], preferred_element_type=F32)
            )

    def add_grads(k_low, pg_then, upd_then):
        at = pl.ds(k_low, 2)
        left = low[at].reshape(2 * rows, width)
        right = pg_then[...].reshape(2 * rows, hidden + 2 * cols)
        acc[0] += lax.dot_general(left, right[:, :hidden], turned, preferred_element_type=F32)
        acc_dec[...] += lax.dot_general(
            left, right[:, hidden:], turned, preferred_element_type=F32
        )
        acc[1] += lax.dot_general(
            upd_then[...].reshape(2 * rows, width),
            act[at].reshape(2 * rows, hidden),
            turned,
            preferred_element_type=F32,
        )

    pg_b[...] = jnp.zeros_like(pg_b)
    upd_b[...] = jnp.zeros_like(upd_b)

    def backward(i, _):
        k = steps - 4 - 4 * i
        back_pair(k + 2, pg_a, upd_a)
        add_grads(jnp.minimum(k + 4, steps - 2), pg_b, upd_b)
        back_pair(k, pg_b, upd_b)
        add_grads(k + 2, pg_a, upd_a)
        return 0

    lax.fori_loop(0, steps // 4, backward, 0)
    add_grads(0, pg_b, upd_b)
    grad_init[...] = state[...]
    final = acc_dec[...] + lax.dot_general(
        low[steps], seen_back[steps], turned, preferred_element_type=F32
    )
    core = place[0]
    spot = place[1]
    slots = keep.shape[0]
    deep = width // slots
    halves = share // cols
    acc_dec[:, :cols] = final[:, :cols] + final[:, cols:]
    in_sum = jnp.sum(in_acc[...], axis=0, keepdims=True)
    out_sum = jnp.sum(out_acc[...], axis=0, keepdims=True)
    kl = 0.5 * jnp.sum(jnp.transpose(kl_acc[...]), axis=0, keepdims=True)
    loglik = -0.5 * jnp.sum(jnp.transpose(sq_acc[...]), axis=0, keepdims=True)
    rest = [out_sum[:, p * cols : (p + 1) * cols] for p in range(width // cols)]
    rest = rest + [loglik, kl]
    rest = rest + [jnp.zeros((8 - halves - len(rest), cols), F32)]
    base = halves * deep
    tile = slots * 8
    for half, out in ((core, keep), (1 - core, send)):
        decs = acc_dec[pl.ds(pl.multiple_of(half * tile, 8), tile), :cols].reshape(slots, 8, cols)
        for s in range(parts):
            q = lax.rem(spot + (parts - s), parts)
            aux = [in_sum[:, s * share + p * cols : s * share + (p + 1) * cols] for p in range(halves)]
            aux = jnp.concatenate(aux + rest, axis=0)
            for p in range(halves):
                block = slice(s * share + p * cols, s * share + (p + 1) * cols)
                out[:, q, p * deep : (p + 1) * deep, :] = acc[half, :, block].reshape(
                    slots, deep, cols
                )
            out[:, q, base : base + 8, :] = decs
            out[:, q, base + 8 : base + 16, :] = jnp.broadcast_to(aux[None], (slots, 8, cols))
    divisor = width * lens + cols * seen
    elbo[...] = (loglik - kl) / divisor


def solve(init, brown, step, lengths, obs_steps, observed, pieces, b_out, dec, prior, diff, place, slots):
    rows, width = init.shape
    steps = brown.shape[0]
    parts = len(pieces)
    share = pieces[0].shape[1]
    hidden = parts * share
    seen, cols = observed.shape[1:]
    vmem = pl.BlockSpec(memory_space=pltpu.VMEM)
    home = pl.BlockSpec(memory_space=pltpu.HBM)
    shape = jax.ShapeDtypeStruct
    ends = jnp.concatenate([step, lengths.astype(F32)])[None]
    packed = jnp.concatenate(
        [
            init,
            b_out[None],
            prior[None],
            diff[None],
            ends,
            obs_steps.T.astype(F32).reshape(seen // 2, 2 * rows),
            jnp.concatenate([dec[:rows], dec[rows:]], axis=1).astype(F32),
        ],
        axis=0,
    )
    payload = shape((slots, parts, width // slots * share // cols + 16, cols), F32)
    outs = (
        payload,
        payload,
        shape((1, rows), F32),
        shape((rows, width), F32),
    )
    return pl.pallas_call(
        series_kernel,
        name="series",
        out_shape=outs,
        in_specs=[home]
        + [vmem] * (2 + parts)
        + [pl.BlockSpec(memory_space=pltpu.SMEM)],
        out_specs=(vmem,) * len(outs),
        scratch_shapes=[
            pltpu.VMEM((steps, rows, hidden), BF16),
            pltpu.VMEM((steps + 1, rows, 2 * cols), BF16),
            pltpu.VMEM((steps + 1, rows, width), BF16),
            pltpu.VMEM((2, rows, hidden + 2 * cols), BF16),
            pltpu.VMEM((2, rows, hidden + 2 * cols), BF16),
            pltpu.VMEM((2, rows, width), BF16),
            pltpu.VMEM((2, rows, width), BF16),
            pltpu.VMEM((steps, rows, width), F32),
            pltpu.VMEM((1, hidden), F32),
            pltpu.VMEM((hidden, width), BF16),
            pltpu.VMEM((hidden + 2 * cols, width), BF16),
            pltpu.VMEM((parts, width, share), BF16),
            pltpu.VMEM((seen, rows, cols), F32),
            pltpu.VMEM((rows, width), F32),
            pltpu.VMEM((rows, rows), F32),
            pltpu.VMEM((rows, cols), F32),
            pltpu.VMEM((8, hidden), F32),
            pltpu.VMEM((8, width), F32),
            pltpu.VMEM((2, width, hidden), F32),
            pltpu.VMEM((width, 2 * cols), F32),
            pltpu.VMEM((steps, rows, width), BF16),
            pltpu.VMEM((width, cols), BF16),
            pltpu.SemaphoreType.DMA,
        ],
        compiler_params=pltpu.CompilerParams(vmem_limit_bytes=48 * 1024 * 1024),
        cost_estimate=pl.CostEstimate(
            flops=12 * steps * rows * width * hidden,
            bytes_accessed=8 * 1024 * 1024,
            transcendentals=steps * rows * hidden,
        ),
    )(
        brown,
        packed,
        jnp.transpose(observed, (1, 0, 2)),
        *pieces,
        place,
    )


def encode_kernel(mine, other, coded):
    total = mine[...] + other[...]
    depth = total.shape[1] - 16

    def scaled_part(part):
        peak = jnp.max(jnp.abs(part), axis=1, keepdims=True)
        power = jnp.floor(jnp.log2(jnp.maximum(peak, 1e-30))) + 1.0
        return part * jnp.exp2(14.0 - power), power

    weights, weights_power = scaled_part(total[:, :depth])
    decs, decs_power = scaled_part(total[:, depth : depth + 8])
    rest, rest_power = scaled_part(total[:, depth + 8 :])
    rest_high = jnp.round(rest)
    rest_low = (rest - rest_high) * 16384.0
    row = lax.broadcasted_iota(jnp.int32, rest.shape, 1)
    powers = jnp.where(row == 0, weights_power, jnp.where(row == 1, decs_power, rest_power))
    full = jnp.concatenate([weights, decs, rest_high, rest_low, powers], axis=1)
    coded[...] = jnp.round(full).astype(jnp.int32).astype(jnp.int16)


def encode(mine, other):
    members, depth, cols = mine.shape
    vmem = pl.BlockSpec(memory_space=pltpu.VMEM)
    return pl.pallas_call(
        encode_kernel,
        name="encode",
        out_shape=jax.ShapeDtypeStruct((members, depth + 16, cols), jnp.int16),
        in_specs=[vmem, vmem],
        out_specs=vmem,
        compiler_params=pltpu.CompilerParams(vmem_limit_bytes=16 * 1024 * 1024),
    )(mine, other)


def sum_kernel(scale, parts, spread, rest):
    depth = spread.shape[1]
    weights = depth - 8
    values = parts[...].astype(jnp.int32).astype(F32)
    units = jnp.exp2(values[:, depth + 16 :] - 14.0) * scale
    main = jnp.sum(values[:, :weights] * units[:, 0:1], axis=0)
    decs = jnp.sum(values[:, weights:depth] * units[:, 1:2], axis=0)
    high, low = values[:, depth : depth + 8], values[:, depth + 8 : depth + 16]
    rest[...] = jnp.sum((high + low * (1.0 / 16384.0)) * units[:, 2:3], axis=0)
    spread[:, :weights] = jnp.broadcast_to(main[None], (spread.shape[0], *main.shape))
    spread[:, weights:] = jnp.broadcast_to(decs[None], (spread.shape[0], *decs.shape))


def sum_parts(parts, slots, scale):
    _, depth, cols = parts.shape
    vmem = pl.BlockSpec(memory_space=pltpu.VMEM)
    return pl.pallas_call(
        functools.partial(sum_kernel, scale),
        name="sum_parts",
        out_shape=(
            jax.ShapeDtypeStruct((slots, depth - 24, cols), F32),
            jax.ShapeDtypeStruct((8, cols), F32),
        ),
        in_specs=[vmem],
        out_specs=(vmem, vmem),
        compiler_params=pltpu.CompilerParams(vmem_limit_bytes=16 * 1024 * 1024),
    )(parts)


def lay_kernel(place, mine, other, w_in, w_out, dec):
    core = place[0]
    slots, depth, cols = mine.shape
    width = w_in.shape[0]
    deep = width // slots

    def lay(low, high):
        for p in range(w_in.shape[1] // cols):
            rows = slice(p * deep, (p + 1) * deep)
            block = slice(p * cols, (p + 1) * cols)
            w_in[:, block] = low[:, rows, :].reshape(width, cols)
            w_out[block, :] = jnp.transpose(high[:, rows, :].reshape(width, cols))
        dec[: slots * 8, :] = low[:, depth - 8 :, :].reshape(slots * 8, cols)
        dec[slots * 8 :, :] = high[:, depth - 8 :, :].reshape(slots * 8, cols)

    pl.when(core == 0)(lambda: lay(mine, other))
    pl.when(core == 1)(lambda: lay(other, mine))


def lay_out(place, mine, other, width, share, cols):
    vmem = pl.BlockSpec(memory_space=pltpu.VMEM)
    shape = jax.ShapeDtypeStruct
    return pl.pallas_call(
        lay_kernel,
        name="lay_out",
        out_shape=(
            shape((width, share), F32),
            shape((share, width), F32),
            shape((width, cols), F32),
        ),
        in_specs=[pl.BlockSpec(memory_space=pltpu.SMEM), vmem, vmem],
        out_specs=(vmem,) * 3,
        compiler_params=pltpu.CompilerParams(vmem_limit_bytes=8 * 1024 * 1024),
    )(place, mine, other)


AXES = ("y", "z", "c", "x")
RING = ("y", "z", "x")


def shifted(array, axis, by):
    count = lax.axis_size(axis)
    return lax.ppermute(array, axis, [(i, (i + by) % count) for i in range(count)])


def on_device(
    init_state,
    brownian,
    step_size,
    lengths,
    obs_steps,
    observed,
    w_in,
    b_in,
    w_out,
    b_out,
    decoder,
    prior_rate,
    diffusion,
):
    width = init_state.shape[1]
    share = w_in.shape[1]
    parts = lax.axis_size("x")
    slots = lax.axis_size("y") * lax.axis_size("z")
    cols = decoder.shape[1]
    core = lax.axis_index("c")
    spot = lax.axis_index("x")

    mine = jnp.concatenate([w_in, w_out, jnp.broadcast_to(b_in[None], (16, share))], axis=0)
    pieces = [mine] + [shifted(mine, "x", by) for by in range(1, parts)]
    place = jnp.stack([core, spot]).astype(jnp.int32)
    keep, send, elbo, grad_init = solve(
        init_state,
        brownian,
        step_size,
        lengths,
        obs_steps,
        observed,
        pieces,
        b_out,
        decoder,
        prior_rate,
        diffusion,
        place,
        slots,
    )
    scale = 1.0 / (init_state.shape[0] * lax.axis_size(AXES))
    members = slots * parts
    other = shifted(send, "c", 1)
    coded = encode(keep.reshape(members, -1, cols), other.reshape(members, -1, cols))
    received = lax.all_to_all(coded, RING, 0, 0, tiled=True)
    spread, rest = sum_parts(received, slots, scale)
    own = lax.all_to_all(spread, ("y", "z"), 0, 0, tiled=True)
    other = shifted(own, "c", 1)
    grad_w_in, grad_w_out, grad_decoder = lay_out(place, own, other, width, share, cols)
    per = share // cols
    end = per + width // cols
    return (
        elbo.reshape(-1),
        jnp.sum(rest[end : end + 2], axis=1),
        grad_w_in,
        rest[:per].reshape(-1),
        grad_w_out,
        rest[per:end].reshape(-1),
        grad_decoder,
        grad_init,
    )


def solution(mesh):
    torus = Mesh(mesh.devices.reshape(4, 4, 2, mesh.shape["mp"]), AXES)
    return jax.shard_map(
        on_device,
        mesh=torus,
        in_specs=(
            P(AXES, None),
            P(None, AXES, None),
            P(AXES),
            P(AXES),
            P(AXES, None),
            P(AXES, None, None),
            P(None, "x"),
            P("x"),
            P("x", None),
            P(),
            P(),
            P(),
            P(),
        ),
        out_specs=(
            P(AXES),
            P(),
            P(None, "x"),
            P("x"),
            P("x", None),
            P(),
            P(),
            P(AXES, None),
        ),
        check_vma=False,
    )
```

```python
import functools

import jax
import jax.numpy as jnp
from jax import lax
from jax.experimental import pallas as pl
from jax.experimental.pallas import tpu as pltpu
from jax.sharding import Mesh
from jax.sharding import PartitionSpec as P

F32 = jnp.float32
BF16 = jnp.bfloat16


def wide(x):
    return jnp.concatenate([x, x], axis=1)


def column(row, rows):
    return jnp.transpose(jnp.broadcast_to(row, (rows, rows)))


def series_kernel(
    brown_home,
    packed,
    obs,
    half_0,
    half_1,
    half_2,
    half_3,
    rest_0,
    rest_1,
    rest_2,
    rest_3,
    place,
    keep,
    send,
    elbo,
    grad_init,
    act,
    seen_back,
    low,
    pg_a,
    pg_b,
    upd_a,
    upd_b,
    scaled,
    b_in,
    w_in,
    w_out,
    w_in_t,
    w_out_t,
    obs_at,
    state,
    kl_acc,
    sq_acc,
    in_acc,
    out_acc,
    acc,
    acc_dec,
    brown,
    dec,
    seen_now,
    moved,
    before,
    done,
):
    fetch = pltpu.make_async_copy(brown_home, brown, done)
    fetch.start()
    steps, rows, width = brown.shape
    halves = (half_0, half_1, half_2, half_3)
    rests = (rest_0, rest_1, rest_2, rest_3)
    parts = len(halves)
    share = half_0.shape[1]
    hidden = parts * share
    cols = dec.shape[1]
    seen = obs.shape[0]
    first, last_row = packed[:rows, :], packed[rows : rows + 8, :]
    b_out, prior, diff = last_row[0:1], last_row[1:2], last_row[2:3]
    step, lens = last_row[3:4, :rows], last_row[3:4, rows:]
    dec_home = packed[rows + 8 :, :].astype(BF16)
    dec[:rows, :] = dec_home[:, :cols]
    dec[rows:, :] = dec_home[:, cols:]

    core = place[0]

    def unpack(ins, outs):
        for q in range(parts):
            block = slice(q * share, (q + 1) * share)
            w_in[q] = ins[q][:width, :]
            w_out[block, :] = outs[q][:width, :]
            w_in_t[block, :] = jnp.transpose(ins[q][:width, :])
            w_out_t[q] = jnp.transpose(outs[q][:width, :])

    pl.when(core == 0)(lambda: unpack(halves, rests))
    pl.when(core == 1)(lambda: unpack(rests, halves))
    for q in range(parts):
        b_in[:, q * share : (q + 1) * share] = halves[q][width:, :].astype(F32)[:1]

    step_b = column(step, rows)
    root_b = jnp.sqrt(step_b)
    lens_b = column(lens, rows)
    inv = 1.0 / diff
    for j in range(seen):
        half = (j % 2) * rows
        obs_at[j] = column(last_row[4 + j // 2 : 5 + j // 2, half : half + rows], rows)
    dec_t = jnp.transpose(dec[...])
    w_in_t[hidden : hidden + cols, :] = dec_t
    w_in_t[hidden + cols : hidden + 2 * cols, :] = dec_t

    state[...] = first
    kl_acc[...] = jnp.zeros_like(kl_acc)
    sq_acc[...] = jnp.zeros_like(sq_acc)
    in_acc[...] = jnp.zeros_like(in_acc)
    out_acc[...] = jnp.zeros_like(out_acc)
    acc[...] = jnp.zeros_like(acc)
    acc_dec[...] = jnp.zeros_like(acc_dec)

    early = 4
    seen_now[...] = jnp.zeros_like(seen_now)
    moved[...] = jnp.broadcast_to(-b_out, (rows, width))
    before[...] = jnp.zeros_like(before)

    def observe_some(k, which, total, squares):
        stamp = k.astype(F32)
        product = seen_now[...]
        for j in which:
            misfit = jnp.where(obs_at[j] == stamp, product - obs[j].astype(F32), 0.0)
            squares = squares + misfit * misfit
            total = total + misfit.astype(BF16).astype(F32)
        return total, squares

    def store_back(total, at):
        high = total.astype(BF16)
        seen_back[at, :, :cols] = high
        seen_back[at, :, cols:] = (total - high.astype(F32)).astype(BF16)

    def observe(k, at):
        total, squares = observe_some(k, range(seen), jnp.zeros((rows, cols), F32), sq_acc[...])
        sq_acc[...] = squares
        store_back(total, at)

    def settle(k):
        at = jnp.maximum(k, 0)
        factor = wide(jnp.where(k.astype(F32) < lens_b, step_b, 0.0))
        residual = (moved[...] + b_out + prior * before[...]) * inv
        scaled[at] = residual * inv
        spent = factor * (residual * residual)
        kl_acc[...] += spent[:, :rows] + spent[:, rows:]

    def forward(k, _):
        now = state[...]
        low_now = now.astype(BF16)
        low[k] = low_now
        live = k.astype(F32) < lens_b
        factor = wide(jnp.where(live, step_b, 0.0))
        noise = wide(jnp.where(live, root_b, 0.0))
        base = now + (factor * b_out + diff * noise * brown[k].astype(F32))
        past = k - 1
        total, squares = observe_some(
            past, range(early), jnp.zeros((rows, cols), F32), sq_acc[...]
        )
        floor = jnp.min((squares + jnp.abs(total)).reshape(rows // 8, 8, cols), axis=0)
        nothing = wide(jnp.minimum(floor, 0.0))[None]
        for q in range(parts):
            block = slice(q * share, (q + 1) * share)
            pre = jnp.dot(low_now, w_in[q], preferred_element_type=F32)
            if q == 0:
                pre = (pre.reshape(rows // 8, 8, share) + (nothing + b_in[:, block])).reshape(
                    rows, share
                )
            else:
                pre = pre + b_in[:, block]
            act[k, :, block] = jnp.tanh(pre).astype(BF16)
        settle(past)
        total, squares = observe_some(past, range(early, seen), total, squares)
        sq_acc[...] = squares
        store_back(total, jnp.maximum(past, 0))
        seen_now[...] = jnp.dot(low_now, dec[...], preferred_element_type=F32)
        product = jnp.dot(act[k], w_out[...], preferred_element_type=F32)
        moved[...] = product
        before[...] = now
        state[...] = base + factor * product
        return 0

    fetch.wait()
    lax.fori_loop(0, steps, forward, 0)
    settle(jnp.int32(steps - 1))
    observe(jnp.int32(steps - 1), steps - 1)
    last = state[...].astype(BF16)
    low[steps] = last
    seen_now[...] = jnp.dot(last, dec[...], preferred_element_type=F32)
    observe(jnp.int32(steps), steps)

    state[...] = jnp.dot(
        seen_back[steps], w_in_t[hidden:, :], preferred_element_type=F32
    )

    turned = (((0,), (0,)), ((), ()))

    def back_pair(k_low, pg_now, upd_now):
        for slot in (1, 0):
            k = k_low + slot
            cot = state[...]
            factor = wide(jnp.where(k.astype(F32) < lens_b, step_b, 0.0))
            pull = scaled[k]
            update = factor * (cot + pull)
            low_up = update.astype(BF16)
            upd_now[slot] = low_up
            out_acc[...] += jnp.sum(update.reshape(rows // 8, 8, width), axis=0)
            for q in range(parts):
                block = slice(q * share, (q + 1) * share)
                a = act[k, :, block].astype(F32)
                pre = jnp.dot(low_up, w_out_t[q], preferred_element_type=F32) * (1.0 - a * a)
                pg_now[slot, :, block] = pre.astype(BF16)
                in_acc[:, block] += jnp.sum(pre.reshape(rows // 8, 8, share), axis=0)
            pg_now[slot, :, hidden:] = seen_back[k]
            state[...] = (
                cot
                + factor * (prior * pull)
                + jnp.dot(pg_now[slot], w_in_t[...], preferred_element_type=F32)
            )

    def add_grads(k_low, pg_then, upd_then):
        at = pl.ds(k_low, 2)
        left = low[at].reshape(2 * rows, width)
        right = pg_then[...].reshape(2 * rows, hidden + 2 * cols)
        acc[0] += lax.dot_general(left, right[:, :hidden], turned, preferred_element_type=F32)
        acc_dec[...] += lax.dot_general(
            left, right[:, hidden:], turned, preferred_element_type=F32
        )
        acc[1] += lax.dot_general(
            upd_then[...].reshape(2 * rows, width),
            act[at].reshape(2 * rows, hidden),
            turned,
            preferred_element_type=F32,
        )

    pg_b[...] = jnp.zeros_like(pg_b)
    upd_b[...] = jnp.zeros_like(upd_b)

    def backward(i, _):
        k = steps - 4 - 4 * i
        back_pair(k + 2, pg_a, upd_a)
        add_grads(jnp.minimum(k + 4, steps - 2), pg_b, upd_b)
        back_pair(k, pg_b, upd_b)
        add_grads(k + 2, pg_a, upd_a)
        return 0

    lax.fori_loop(0, steps // 4, backward, 0)
    add_grads(0, pg_b, upd_b)
    grad_init[...] = state[...]
    final = acc_dec[...] + lax.dot_general(
        low[steps], seen_back[steps], turned, preferred_element_type=F32
    )
    spot = place[1]
    slots = keep.shape[0]
    deep = width // slots
    lanes = share // cols
    acc_dec[:, :cols] = final[:, :cols] + final[:, cols:]
    in_sum = jnp.sum(in_acc[...], axis=0, keepdims=True)
    out_sum = jnp.sum(out_acc[...], axis=0, keepdims=True)
    kl = 0.5 * jnp.sum(jnp.transpose(kl_acc[...]), axis=0, keepdims=True)
    loglik = -0.5 * jnp.sum(jnp.transpose(sq_acc[...]), axis=0, keepdims=True)
    rest = [out_sum[:, p * cols : (p + 1) * cols] for p in range(width // cols)]
    rest = rest + [loglik, kl]
    rest = rest + [jnp.zeros((8 - lanes - len(rest), cols), F32)]
    base = lanes * deep
    tile = slots * 8
    for half, out in ((core, keep), (1 - core, send)):
        decs = acc_dec[pl.ds(pl.multiple_of(half * tile, 8), tile), :cols].reshape(slots, 8, cols)
        for s in range(parts):
            q = lax.rem(spot + (parts - s), parts)
            aux = [in_sum[:, s * share + p * cols : s * share + (p + 1) * cols] for p in range(lanes)]
            aux = jnp.concatenate(aux + rest, axis=0)
            for p in range(lanes):
                block = slice(s * share + p * cols, s * share + (p + 1) * cols)
                out[:, q, p * deep : (p + 1) * deep, :] = acc[half, :, block].reshape(
                    slots, deep, cols
                )
            out[:, q, base : base + 8, :] = decs
            out[:, q, base + 8 : base + 16, :] = jnp.broadcast_to(aux[None], (slots, 8, cols))
    divisor = width * lens + cols * seen
    elbo[...] = (loglik - kl) / divisor


def solve(init, brown, step, lengths, obs_steps, observed, halves, rests, b_out, dec, prior, diff, place, slots):
    rows, width = init.shape
    steps = brown.shape[0]
    parts = len(halves)
    share = halves[0].shape[1]
    hidden = parts * share
    seen, cols = observed.shape[1:]
    vmem = pl.BlockSpec(memory_space=pltpu.VMEM)
    home = pl.BlockSpec(memory_space=pltpu.HBM)
    shape = jax.ShapeDtypeStruct
    ends = jnp.concatenate([step, lengths.astype(F32)])[None]
    packed = jnp.concatenate(
        [
            init,
            b_out[None],
            prior[None],
            diff[None],
            ends,
            obs_steps.T.astype(F32).reshape(seen // 2, 2 * rows),
            jnp.concatenate([dec[:rows], dec[rows:]], axis=1).astype(F32),
        ],
        axis=0,
    )
    payload = shape((slots, parts, width // slots * share // cols + 16, cols), F32)
    outs = (
        payload,
        payload,
        shape((1, rows), F32),
        shape((rows, width), F32),
    )
    return pl.pallas_call(
        series_kernel,
        name="series",
        out_shape=outs,
        in_specs=[home]
        + [vmem] * (2 + 2 * parts)
        + [pl.BlockSpec(memory_space=pltpu.SMEM)],
        out_specs=(vmem,) * len(outs),
        scratch_shapes=[
            pltpu.VMEM((steps, rows, hidden), BF16),
            pltpu.VMEM((steps + 1, rows, 2 * cols), BF16),
            pltpu.VMEM((steps + 1, rows, width), BF16),
            pltpu.VMEM((2, rows, hidden + 2 * cols), BF16),
            pltpu.VMEM((2, rows, hidden + 2 * cols), BF16),
            pltpu.VMEM((2, rows, width), BF16),
            pltpu.VMEM((2, rows, width), BF16),
            pltpu.VMEM((steps, rows, width), F32),
            pltpu.VMEM((1, hidden), F32),
            pltpu.VMEM((parts, width, share), BF16),
            pltpu.VMEM((hidden, width), BF16),
            pltpu.VMEM((hidden + 2 * cols, width), BF16),
            pltpu.VMEM((parts, width, share), BF16),
            pltpu.VMEM((seen, rows, cols), F32),
            pltpu.VMEM((rows, width), F32),
            pltpu.VMEM((rows, rows), F32),
            pltpu.VMEM((rows, cols), F32),
            pltpu.VMEM((8, hidden), F32),
            pltpu.VMEM((8, width), F32),
            pltpu.VMEM((2, width, hidden), F32),
            pltpu.VMEM((width, 2 * cols), F32),
            pltpu.VMEM((steps, rows, width), BF16),
            pltpu.VMEM((width, cols), BF16),
            pltpu.VMEM((rows, cols), F32),
            pltpu.VMEM((rows, width), F32),
            pltpu.VMEM((rows, width), F32),
            pltpu.SemaphoreType.DMA,
        ],
        compiler_params=pltpu.CompilerParams(vmem_limit_bytes=48 * 1024 * 1024),
        cost_estimate=pl.CostEstimate(
            flops=12 * steps * rows * width * hidden,
            bytes_accessed=8 * 1024 * 1024,
            transcendentals=steps * rows * hidden,
        ),
    )(
        brown,
        packed,
        jnp.transpose(observed, (1, 0, 2)),
        *halves,
        *rests,
        place,
    )


def encode_kernel(mine, other, coded):
    total = mine[...] + other[...]
    depth = total.shape[1] - 16

    def scaled_part(part):
        peak = jnp.max(jnp.abs(part), axis=1, keepdims=True)
        power = jnp.floor(jnp.log2(jnp.maximum(peak, 1e-30))) + 1.0
        return part * jnp.exp2(14.0 - power), power

    weights, weights_power = scaled_part(total[:, :depth])
    decs, decs_power = scaled_part(total[:, depth : depth + 8])
    rest, rest_power = scaled_part(total[:, depth + 8 :])
    rest_high = jnp.round(rest)
    rest_low = (rest - rest_high) * 16384.0
    row = lax.broadcasted_iota(jnp.int32, rest.shape, 1)
    powers = jnp.where(row == 0, weights_power, jnp.where(row == 1, decs_power, rest_power))
    full = jnp.concatenate([weights, decs, rest_high, rest_low, powers], axis=1)
    coded[...] = jnp.round(full).astype(jnp.int32).astype(jnp.int16)


def encode(mine, other):
    members, depth, cols = mine.shape
    vmem = pl.BlockSpec(memory_space=pltpu.VMEM)
    return pl.pallas_call(
        encode_kernel,
        name="encode",
        out_shape=jax.ShapeDtypeStruct((members, depth + 16, cols), jnp.int16),
        in_specs=[vmem, vmem],
        out_specs=vmem,
        compiler_params=pltpu.CompilerParams(vmem_limit_bytes=16 * 1024 * 1024),
    )(mine, other)


def sum_kernel(scale, parts, spread, rest):
    depth = spread.shape[1]
    weights = depth - 8
    values = parts[...].astype(jnp.int32).astype(F32)
    units = jnp.exp2(values[:, depth + 16 :] - 14.0) * scale
    main = jnp.sum(values[:, :weights] * units[:, 0:1], axis=0)
    decs = jnp.sum(values[:, weights:depth] * units[:, 1:2], axis=0)
    high, low = values[:, depth : depth + 8], values[:, depth + 8 : depth + 16]
    rest[...] = jnp.sum((high + low * (1.0 / 16384.0)) * units[:, 2:3], axis=0)
    spread[:, :weights] = jnp.broadcast_to(main[None], (spread.shape[0], *main.shape))
    spread[:, weights:] = jnp.broadcast_to(decs[None], (spread.shape[0], *decs.shape))


def sum_parts(parts, slots, scale):
    _, depth, cols = parts.shape
    vmem = pl.BlockSpec(memory_space=pltpu.VMEM)
    return pl.pallas_call(
        functools.partial(sum_kernel, scale),
        name="sum_parts",
        out_shape=(
            jax.ShapeDtypeStruct((slots, depth - 24, cols), F32),
            jax.ShapeDtypeStruct((8, cols), F32),
        ),
        in_specs=[vmem],
        out_specs=(vmem, vmem),
        compiler_params=pltpu.CompilerParams(vmem_limit_bytes=16 * 1024 * 1024),
    )(parts)


def lay_kernel(place, mine, other, w_in, w_out, dec):
    core = place[0]
    slots, depth, cols = mine.shape
    width = w_in.shape[0]
    deep = width // slots

    def lay(low, high):
        for p in range(w_in.shape[1] // cols):
            rows = slice(p * deep, (p + 1) * deep)
            block = slice(p * cols, (p + 1) * cols)
            w_in[:, block] = low[:, rows, :].reshape(width, cols)
            w_out[block, :] = jnp.transpose(high[:, rows, :].reshape(width, cols))
        dec[: slots * 8, :] = low[:, depth - 8 :, :].reshape(slots * 8, cols)
        dec[slots * 8 :, :] = high[:, depth - 8 :, :].reshape(slots * 8, cols)

    pl.when(core == 0)(lambda: lay(mine, other))
    pl.when(core == 1)(lambda: lay(other, mine))


def lay_out(place, mine, other, width, share, cols):
    vmem = pl.BlockSpec(memory_space=pltpu.VMEM)
    shape = jax.ShapeDtypeStruct
    return pl.pallas_call(
        lay_kernel,
        name="lay_out",
        out_shape=(
            shape((width, share), F32),
            shape((share, width), F32),
            shape((width, cols), F32),
        ),
        in_specs=[pl.BlockSpec(memory_space=pltpu.SMEM), vmem, vmem],
        out_specs=(vmem,) * 3,
        compiler_params=pltpu.CompilerParams(vmem_limit_bytes=8 * 1024 * 1024),
    )(place, mine, other)


AXES = ("y", "z", "c", "x")
RING = ("y", "z", "x")


def shifted(array, axis, by):
    count = lax.axis_size(axis)
    return lax.ppermute(array, axis, [(i, (i + by) % count) for i in range(count)])


def on_device(
    init_state,
    brownian,
    step_size,
    lengths,
    obs_steps,
    observed,
    w_in,
    b_in,
    w_out,
    b_out,
    decoder,
    prior_rate,
    diffusion,
):
    width = init_state.shape[1]
    share = w_in.shape[1]
    parts = lax.axis_size("x")
    slots = lax.axis_size("y") * lax.axis_size("z")
    cols = decoder.shape[1]
    core = lax.axis_index("c")
    spot = lax.axis_index("x")

    bias_rows = jnp.broadcast_to(b_in[None], (16, share))
    half = jnp.concatenate([jnp.where(core == 0, w_in, w_out), bias_rows], axis=0)
    halves = [half] + [shifted(half, "x", by) for by in range(1, parts)]
    rests = [jnp.where(core == 0, w_out, w_in)] + [shifted(got, "c", 1) for got in halves[1:]]
    place = jnp.stack([core, spot]).astype(jnp.int32)
    keep, send, elbo, grad_init = solve(
        init_state,
        brownian,
        step_size,
        lengths,
        obs_steps,
        observed,
        halves,
        rests,
        b_out,
        decoder,
        prior_rate,
        diffusion,
        place,
        slots,
    )
    scale = 1.0 / (init_state.shape[0] * lax.axis_size(AXES))
    members = slots * parts
    other = shifted(send, "c", 1)
    coded = encode(keep.reshape(members, -1, cols), other.reshape(members, -1, cols))
    received = lax.all_to_all(coded, RING, 0, 0, tiled=True)
    spread, rest = sum_parts(received, slots, scale)
    own = lax.all_to_all(spread, ("y", "z"), 0, 0, tiled=True)
    other = shifted(own, "c", 1)
    grad_w_in, grad_w_out, grad_decoder = lay_out(place, own, other, width, share, cols)
    per = share // cols
    end = per + width // cols
    return (
        elbo.reshape(-1),
        jnp.sum(rest[end : end + 2], axis=1),
        grad_w_in,
        rest[:per].reshape(-1),
        grad_w_out,
        rest[per:end].reshape(-1),
        grad_decoder,
        grad_init,
    )


def solution(mesh):
    torus = Mesh(mesh.devices.reshape(4, 4, 2, mesh.shape["mp"]), AXES)
    return jax.shard_map(
        on_device,
        mesh=torus,
        in_specs=(
            P(AXES, None),
            P(None, AXES, None),
            P(AXES),
            P(AXES),
            P(AXES, None),
            P(AXES, None, None),
            P(None, "x"),
            P("x"),
            P("x", None),
            P(),
            P(),
            P(),
            P(),
        ),
        out_specs=(
            P(AXES),
            P(),
            P(None, "x"),
            P("x"),
            P("x", None),
            P(),
            P(),
            P(AXES, None),
        ),
        check_vma=False,
    )
```

```python
import functools

import jax
import jax.numpy as jnp
from jax import lax
from jax.experimental import pallas as pl
from jax.experimental.pallas import tpu as pltpu
from jax.sharding import Mesh
from jax.sharding import PartitionSpec as P

F32 = jnp.float32
BF16 = jnp.bfloat16


def wide(x):
    return jnp.concatenate([x, x], axis=1)


def column(row, rows):
    return jnp.transpose(jnp.broadcast_to(row, (rows, rows)))


def series_kernel(
    brown,
    packed,
    obs,
    half_0,
    half_1,
    half_2,
    half_3,
    rest_0,
    rest_1,
    rest_2,
    rest_3,
    place,
    keep,
    send,
    elbo,
    grad_init,
    act,
    seen_back,
    low,
    pg_a,
    pg_b,
    upd_a,
    upd_b,
    scaled,
    b_in,
    w_in,
    w_out,
    w_in_t,
    w_out_t,
    obs_at,
    state,
    kl_acc,
    sq_acc,
    in_acc,
    out_acc,
    acc,
    acc_dec,
    dec,
    seen_now,
    moved,
    before,
):
    steps, rows, width = brown.shape
    halves = (half_0, half_1, half_2, half_3)
    rests = (rest_0, rest_1, rest_2, rest_3)
    parts = len(halves)
    share = half_0.shape[1]
    hidden = parts * share
    cols = dec.shape[1]
    seen = obs.shape[0]
    first, last_row = packed[:rows, :], packed[rows : rows + 8, :]
    b_out, prior, diff = last_row[0:1], last_row[1:2], last_row[2:3]
    step, lens = last_row[3:4, :rows], last_row[3:4, rows:]
    dec_home = packed[rows + 8 :, :].astype(BF16)
    dec[:rows, :] = dec_home[:, :cols]
    dec[rows:, :] = dec_home[:, cols:]

    core = place[0]

    def unpack(ins, outs):
        for q in range(parts):
            block = slice(q * share, (q + 1) * share)
            w_in[q] = ins[q][:width, :]
            w_out[block, :] = outs[q][:width, :]
            w_in_t[block, :] = jnp.transpose(ins[q][:width, :])
            w_out_t[q] = jnp.transpose(outs[q][:width, :])

    pl.when(core == 0)(lambda: unpack(halves, rests))
    pl.when(core == 1)(lambda: unpack(rests, halves))
    for q in range(parts):
        b_in[:, q * share : (q + 1) * share] = halves[q][width:, :].astype(F32)[:1]

    step_b = column(step, rows)
    root_b = jnp.sqrt(step_b)
    lens_b = column(lens, rows)
    inv = 1.0 / diff
    for j in range(seen):
        half = (j % 2) * rows
        obs_at[j] = column(last_row[4 + j // 2 : 5 + j // 2, half : half + rows], rows)
    dec_t = jnp.transpose(dec[...])
    w_in_t[hidden : hidden + cols, :] = dec_t
    w_in_t[hidden + cols : hidden + 2 * cols, :] = dec_t

    state[...] = first
    kl_acc[...] = jnp.zeros_like(kl_acc)
    sq_acc[...] = jnp.zeros_like(sq_acc)
    in_acc[...] = jnp.zeros_like(in_acc)
    out_acc[...] = jnp.zeros_like(out_acc)
    acc[...] = jnp.zeros_like(acc)
    acc_dec[...] = jnp.zeros_like(acc_dec)

    early = 4
    seen_now[...] = jnp.zeros_like(seen_now)
    moved[...] = jnp.broadcast_to(-b_out, (rows, width))
    before[...] = jnp.zeros_like(before)

    def observe_some(k, which, total, squares):
        stamp = k.astype(F32)
        product = seen_now[...]
        for j in which:
            misfit = jnp.where(obs_at[j] == stamp, product - obs[j].astype(F32), 0.0)
            squares = squares + misfit * misfit
            total = total + misfit.astype(BF16).astype(F32)
        return total, squares

    def store_back(total, at):
        high = total.astype(BF16)
        seen_back[at, :, :cols] = high
        seen_back[at, :, cols:] = (total - high.astype(F32)).astype(BF16)

    def observe(k, at):
        total, squares = observe_some(k, range(seen), jnp.zeros((rows, cols), F32), sq_acc[...])
        sq_acc[...] = squares
        store_back(total, at)

    def settle(k):
        at = jnp.maximum(k, 0)
        factor = wide(jnp.where(k.astype(F32) < lens_b, step_b, 0.0))
        residual = (moved[...] + b_out + prior * before[...]) * inv
        scaled[at] = residual * inv
        spent = factor * (residual * residual)
        kl_acc[...] += spent[:, :rows] + spent[:, rows:]

    def forward(k, _):
        now = state[...]
        low_now = now.astype(BF16)
        low[k] = low_now
        live = k.astype(F32) < lens_b
        factor = wide(jnp.where(live, step_b, 0.0))
        noise = wide(jnp.where(live, root_b, 0.0))
        base = now + (factor * b_out + diff * noise * brown[k].astype(F32))
        past = k - 1
        total, squares = observe_some(
            past, range(early), jnp.zeros((rows, cols), F32), sq_acc[...]
        )
        floor = jnp.min((squares + jnp.abs(total)).reshape(rows // 8, 8, cols), axis=0)
        nothing = wide(jnp.minimum(floor, 0.0))[None]
        for q in range(parts):
            block = slice(q * share, (q + 1) * share)
            pre = jnp.dot(low_now, w_in[q], preferred_element_type=F32)
            if q == 0:
                pre = (pre.reshape(rows // 8, 8, share) + (nothing + b_in[:, block])).reshape(
                    rows, share
                )
            else:
                pre = pre + b_in[:, block]
            act[k, :, block] = jnp.tanh(pre).astype(BF16)
        settle(past)
        total, squares = observe_some(past, range(early, seen), total, squares)
        sq_acc[...] = squares
        store_back(total, jnp.maximum(past, 0))
        seen_now[...] = jnp.dot(low_now, dec[...], preferred_element_type=F32)
        product = jnp.dot(act[k], w_out[...], preferred_element_type=F32)
        moved[...] = product
        before[...] = now
        state[...] = base + factor * product
        return 0

    lax.fori_loop(0, steps, forward, 0)
    settle(jnp.int32(steps - 1))
    observe(jnp.int32(steps - 1), steps - 1)
    last = state[...].astype(BF16)
    low[steps] = last
    seen_now[...] = jnp.dot(last, dec[...], preferred_element_type=F32)
    observe(jnp.int32(steps), steps)

    state[...] = jnp.dot(
        seen_back[steps], w_in_t[hidden:, :], preferred_element_type=F32
    )

    turned = (((0,), (0,)), ((), ()))

    def back_pair(k_low, pg_now, upd_now):
        for slot in (1, 0):
            k = k_low + slot
            cot = state[...]
            factor = wide(jnp.where(k.astype(F32) < lens_b, step_b, 0.0))
            pull = scaled[k]
            update = factor * (cot + pull)
            low_up = update.astype(BF16)
            upd_now[slot] = low_up
            out_acc[...] += jnp.sum(update.reshape(rows // 8, 8, width), axis=0)
            for q in range(parts):
                block = slice(q * share, (q + 1) * share)
                a = act[k, :, block].astype(F32)
                pre = jnp.dot(low_up, w_out_t[q], preferred_element_type=F32) * (1.0 - a * a)
                pg_now[slot, :, block] = pre.astype(BF16)
                in_acc[:, block] += jnp.sum(pre.reshape(rows // 8, 8, share), axis=0)
            pg_now[slot, :, hidden:] = seen_back[k]
            state[...] = (
                cot
                + factor * (prior * pull)
                + jnp.dot(pg_now[slot], w_in_t[...], preferred_element_type=F32)
            )

    def add_grads(k_low, pg_then, upd_then):
        at = pl.ds(k_low, 2)
        right = low[at].reshape(2 * rows, width)
        left = pg_then[...].reshape(2 * rows, hidden + 2 * cols)
        acc[0] += lax.dot_general(left[:, :hidden], right, turned, preferred_element_type=F32)
        acc_dec[...] += lax.dot_general(
            left[:, hidden:], right, turned, preferred_element_type=F32
        )
        acc[1] += lax.dot_general(
            act[at].reshape(2 * rows, hidden),
            upd_then[...].reshape(2 * rows, width),
            turned,
            preferred_element_type=F32,
        )

    pg_b[...] = jnp.zeros_like(pg_b)
    upd_b[...] = jnp.zeros_like(upd_b)

    def backward(i, _):
        k = steps - 4 - 4 * i
        back_pair(k + 2, pg_a, upd_a)
        add_grads(jnp.minimum(k + 4, steps - 2), pg_b, upd_b)
        back_pair(k, pg_b, upd_b)
        add_grads(k + 2, pg_a, upd_a)
        return 0

    lax.fori_loop(0, steps // 4, backward, 0, unroll=2)
    add_grads(0, pg_b, upd_b)
    grad_init[...] = state[...]
    final = acc_dec[...] + lax.dot_general(
        seen_back[steps], low[steps], turned, preferred_element_type=F32
    )
    spot = place[1]
    lanes = share // cols
    blocks, depth, _ = keep.shape
    slots = width * lanes // depth
    deep = width // slots
    members = slots * parts
    tile = slots * 8
    acc_dec[:, :cols] = jnp.transpose(final[:cols, :] + final[cols:, :])
    in_sum = jnp.sum(in_acc[...], axis=0, keepdims=True)
    out_sum = jnp.sum(out_acc[...], axis=0, keepdims=True)
    kl = 0.5 * jnp.sum(jnp.transpose(kl_acc[...]), axis=0, keepdims=True)
    loglik = -0.5 * jnp.sum(jnp.transpose(sq_acc[...]), axis=0, keepdims=True)
    rest = [out_sum[:, p * cols : (p + 1) * cols] for p in range(width // cols)]
    rest = rest + [loglik, kl]
    rest = rest + [jnp.zeros((8 - lanes - len(rest), cols), F32)]
    for half, out in ((core, keep), (1 - core, send)):
        decs = acc_dec[pl.ds(pl.multiple_of(half * tile, 8), tile), :cols]
        out[members : members + tile // depth] = decs.reshape(tile // depth, depth, cols)
        for s in range(parts):
            q = lax.rem(spot + (parts - s), parts)
            at = pl.ds(q * slots, slots)
            for p in range(lanes):
                block = slice(s * share, (s + 1) * share)
                out[at, p * deep : (p + 1) * deep, :] = acc[
                    half, block, p * cols : (p + 1) * cols
                ].reshape(slots, deep, cols)
            aux = [in_sum[:, s * share + p * cols : s * share + (p + 1) * cols] for p in range(lanes)]
            out[blocks - 1, pl.ds(pl.multiple_of(q * 8, 8), 8), :] = jnp.concatenate(
                aux + rest, axis=0
            )

    divisor = width * lens + cols * seen
    elbo[...] = (loglik - kl) / divisor


def solve(init, brown, step, lengths, obs_steps, observed, halves, rests, b_out, dec, prior, diff, place, slots):
    rows, width = init.shape
    steps = brown.shape[0]
    parts = len(halves)
    share = halves[0].shape[1]
    hidden = parts * share
    seen, cols = observed.shape[1:]
    vmem = pl.BlockSpec(memory_space=pltpu.VMEM)
    shape = jax.ShapeDtypeStruct
    ends = jnp.concatenate([step, lengths.astype(F32)])[None]
    packed = jnp.concatenate(
        [
            init,
            b_out[None],
            prior[None],
            diff[None],
            ends,
            obs_steps.T.astype(F32).reshape(seen // 2, 2 * rows),
            jnp.concatenate([dec[:rows], dec[rows:]], axis=1).astype(F32),
        ],
        axis=0,
    )
    depth = width // slots * share // cols
    payload = shape((slots * parts + slots * 8 // depth + parts * 8 // depth, depth, cols), F32)
    outs = (
        payload,
        payload,
        shape((1, rows), F32),
        shape((rows, width), F32),
    )
    return pl.pallas_call(
        series_kernel,
        name="series",
        out_shape=outs,
        in_specs=[vmem] * (3 + 2 * parts)
        + [pl.BlockSpec(memory_space=pltpu.SMEM)],
        out_specs=(vmem,) * len(outs),
        scratch_shapes=[
            pltpu.VMEM((steps, rows, hidden), BF16),
            pltpu.VMEM((steps + 1, rows, 2 * cols), BF16),
            pltpu.VMEM((steps + 1, rows, width), BF16),
            pltpu.VMEM((2, rows, hidden + 2 * cols), BF16),
            pltpu.VMEM((2, rows, hidden + 2 * cols), BF16),
            pltpu.VMEM((2, rows, width), BF16),
            pltpu.VMEM((2, rows, width), BF16),
            pltpu.VMEM((steps, rows, width), F32),
            pltpu.VMEM((1, hidden), F32),
            pltpu.VMEM((parts, width, share), BF16),
            pltpu.VMEM((hidden, width), BF16),
            pltpu.VMEM((hidden + 2 * cols, width), BF16),
            pltpu.VMEM((parts, width, share), BF16),
            pltpu.VMEM((seen, rows, cols), F32),
            pltpu.VMEM((rows, width), F32),
            pltpu.VMEM((rows, rows), F32),
            pltpu.VMEM((rows, cols), F32),
            pltpu.VMEM((8, hidden), F32),
            pltpu.VMEM((8, width), F32),
            pltpu.VMEM((2, hidden, width), F32),
            pltpu.VMEM((2 * cols, width), F32),
            pltpu.VMEM((width, cols), BF16),
            pltpu.VMEM((rows, cols), F32),
            pltpu.VMEM((rows, width), F32),
            pltpu.VMEM((rows, width), F32),
        ],
        compiler_params=pltpu.CompilerParams(
            vmem_limit_bytes=40 * 1024 * 1024,
        ),
        cost_estimate=pl.CostEstimate(
            flops=12 * steps * rows * width * hidden,
            bytes_accessed=8 * 1024 * 1024,
            transcendentals=steps * rows * hidden,
        ),
    )(
        brown,
        packed,
        jnp.transpose(observed, (1, 0, 2)),
        *halves,
        *rests,
        place,
    )


def encode_kernel(slots, parts, mine, other, coded):
    depth, cols = mine.shape[1:]
    members = slots * parts
    decs_end = members + slots * 8 // depth
    total = mine[...] + other[...]

    def scaled_part(part):
        peak = jnp.max(jnp.abs(part), axis=1, keepdims=True)
        power = jnp.floor(jnp.log2(jnp.maximum(peak, 1e-30))) + 1.0
        return part * jnp.exp2(14.0 - power), power

    def over_slots(part):
        full = jnp.broadcast_to(part[:, None], (parts, slots, *part.shape[1:]))
        return full.reshape(members, *part.shape[1:])

    def over_parts(part):
        full = jnp.broadcast_to(part[None], (parts, *part.shape))
        return full.reshape(members, *part.shape[1:])

    weights, weights_power = scaled_part(total[:members])
    decs, decs_power = scaled_part(total[members:decs_end].reshape(slots, 8, cols))
    rest, rest_power = scaled_part(total[decs_end:].reshape(parts, 8, cols))
    rest_high = jnp.round(rest)
    rest_low = (rest - rest_high) * 16384.0
    row = lax.broadcasted_iota(jnp.int32, (members, 8, cols), 1)
    rest_low = jnp.where(row == 6, over_slots(jnp.broadcast_to(rest_power, rest.shape)), over_slots(rest_low))
    decs_power = over_parts(jnp.broadcast_to(decs_power, decs.shape))
    rest_high = jnp.where(row == 6, weights_power, jnp.where(row == 7, decs_power, over_slots(rest_high)))
    full = jnp.concatenate([weights, over_parts(decs), rest_high, rest_low], axis=1)
    coded[...] = jnp.round(full).astype(jnp.int32).astype(jnp.int16)


def encode(mine, other, slots, parts):
    depth, cols = mine.shape[1:]
    vmem = pl.BlockSpec(memory_space=pltpu.VMEM)
    return pl.pallas_call(
        functools.partial(encode_kernel, slots, parts),
        name="encode",
        out_shape=jax.ShapeDtypeStruct((slots * parts, depth + 24, cols), jnp.int16),
        in_specs=[vmem, vmem],
        out_specs=vmem,
        compiler_params=pltpu.CompilerParams(vmem_limit_bytes=16 * 1024 * 1024),
    )(mine, other)


def sum_kernel(scale, parts, spread, rest):
    depth = spread.shape[1]
    weights = depth - 8
    values = parts[...].astype(jnp.int32).astype(F32)
    high, low = values[:, depth : depth + 8], values[:, depth + 8 : depth + 16]

    def unit(row):
        return jnp.exp2(row - 14.0) * scale

    main = jnp.sum(values[:, :weights] * unit(high[:, 6:7]), axis=0)
    decs = jnp.sum(values[:, weights:depth] * unit(high[:, 7:8]), axis=0)
    rest[...] = jnp.sum((high + low * (1.0 / 16384.0)) * unit(low[:, 6:7]), axis=0)
    spread[:, :weights] = jnp.broadcast_to(main[None], (spread.shape[0], *main.shape))
    spread[:, weights:] = jnp.broadcast_to(decs[None], (spread.shape[0], *decs.shape))


def sum_parts(parts, slots, scale):
    _, depth, cols = parts.shape
    vmem = pl.BlockSpec(memory_space=pltpu.VMEM)
    return pl.pallas_call(
        functools.partial(sum_kernel, scale),
        name="sum_parts",
        out_shape=(
            jax.ShapeDtypeStruct((slots, depth - 16, cols), F32),
            jax.ShapeDtypeStruct((8, cols), F32),
        ),
        in_specs=[vmem],
        out_specs=(vmem, vmem),
        compiler_params=pltpu.CompilerParams(vmem_limit_bytes=16 * 1024 * 1024),
    )(parts)


def lay_kernel(place, mine, other, w_in, w_out, dec):
    core = place[0]
    slots, depth, cols = mine.shape
    width = w_in.shape[0]
    deep = width // slots

    def lay(low, high):
        for p in range(w_in.shape[1] // cols):
            rows = slice(p * deep, (p + 1) * deep)
            block = slice(p * cols, (p + 1) * cols)
            w_in[block, :] = jnp.transpose(low[:, rows, :].reshape(width, cols))
            w_out[:, block] = high[:, rows, :].reshape(width, cols)
        dec[: slots * 8, :] = low[:, depth - 8 :, :].reshape(slots * 8, cols)
        dec[slots * 8 :, :] = high[:, depth - 8 :, :].reshape(slots * 8, cols)

    pl.when(core == 0)(lambda: lay(mine, other))
    pl.when(core == 1)(lambda: lay(other, mine))


def lay_out(place, mine, other, width, share, cols):
    vmem = pl.BlockSpec(memory_space=pltpu.VMEM)
    shape = jax.ShapeDtypeStruct
    return pl.pallas_call(
        lay_kernel,
        name="lay_out",
        out_shape=(
            shape((width, share), F32),
            shape((share, width), F32),
            shape((width, cols), F32),
        ),
        in_specs=[pl.BlockSpec(memory_space=pltpu.SMEM), vmem, vmem],
        out_specs=(vmem,) * 3,
        compiler_params=pltpu.CompilerParams(vmem_limit_bytes=8 * 1024 * 1024),
    )(place, mine, other)


AXES = ("y", "z", "c", "x")
RING = ("x", "y", "z")


def shifted(array, axis, by):
    count = lax.axis_size(axis)
    return lax.ppermute(array, axis, [(i, (i + by) % count) for i in range(count)])


def on_device(
    init_state,
    brownian,
    step_size,
    lengths,
    obs_steps,
    observed,
    w_in,
    b_in,
    w_out,
    b_out,
    decoder,
    prior_rate,
    diffusion,
):
    width = init_state.shape[1]
    share = w_in.shape[1]
    parts = lax.axis_size("x")
    slots = lax.axis_size("y") * lax.axis_size("z")
    cols = decoder.shape[1]
    core = lax.axis_index("c")
    spot = lax.axis_index("x")

    bias_rows = jnp.broadcast_to(b_in[None], (16, share))
    half = jnp.concatenate([jnp.where(core == 0, w_in, w_out), bias_rows], axis=0)
    halves = [half] + [shifted(half, "x", by) for by in range(1, parts)]
    rests = [jnp.where(core == 0, w_out, w_in)] + [shifted(got, "c", 1) for got in halves[1:]]
    place = jnp.stack([core, spot]).astype(jnp.int32)
    keep, send, elbo, grad_init = solve(
        init_state,
        brownian,
        step_size,
        lengths,
        obs_steps,
        observed,
        halves,
        rests,
        b_out,
        decoder,
        prior_rate,
        diffusion,
        place,
        slots,
    )
    scale = 1.0 / (init_state.shape[0] * lax.axis_size(AXES))
    coded = encode(keep, shifted(send, "c", 1), slots, parts)
    received = lax.all_to_all(coded, RING, 0, 0, tiled=True)
    spread, rest = sum_parts(received, slots, scale)
    own = lax.all_to_all(spread, ("y", "z"), 0, 0, tiled=True)
    other = shifted(own, "c", 1)
    grad_w_in, grad_w_out, grad_decoder = lay_out(place, own, other, width, share, cols)
    per = share // cols
    end = per + width // cols
    return (
        elbo.reshape(-1),
        jnp.sum(rest[end : end + 2], axis=1),
        grad_w_in,
        rest[:per].reshape(-1),
        grad_w_out,
        rest[per:end].reshape(-1),
        grad_decoder,
        grad_init,
    )


def solution(mesh):
    torus = Mesh(mesh.devices.reshape(4, 4, 2, mesh.shape["mp"]), AXES)
    return jax.shard_map(
        on_device,
        mesh=torus,
        in_specs=(
            P(AXES, None),
            P(None, AXES, None),
            P(AXES),
            P(AXES),
            P(AXES, None),
            P(AXES, None, None),
            P(None, "x"),
            P("x"),
            P("x", None),
            P(),
            P(),
            P(),
            P(),
        ),
        out_specs=(
            P(AXES),
            P(),
            P(None, "x"),
            P("x"),
            P("x", None),
            P(),
            P(),
            P(AXES, None),
        ),
        check_vma=False,
    )
```

```python
import functools

import jax
import jax.numpy as jnp
from jax import lax
from jax.experimental import pallas as pl
from jax.experimental.pallas import tpu as pltpu
from jax.sharding import Mesh
from jax.sharding import PartitionSpec as P

F32 = jnp.float32
BF16 = jnp.bfloat16


def wide(x):
    return jnp.concatenate([x, x], axis=1)


def column(row, rows):
    return jnp.transpose(jnp.broadcast_to(row, (rows, rows)))


def series_kernel(
    brown_home,
    packed,
    vectors,
    dec_home,
    obs,
    half_0,
    half_1,
    half_2,
    half_3,
    rest_0,
    rest_1,
    rest_2,
    rest_3,
    place,
    keep,
    send,
    elbo,
    grad_init,
    act,
    seen_back,
    low,
    pg_a,
    pg_b,
    upd_a,
    upd_b,
    scaled,
    b_in,
    w_in,
    w_out,
    w_in_t,
    w_out_t,
    obs_at,
    state,
    kl_acc,
    sq_acc,
    in_acc,
    out_acc,
    acc,
    acc_dec,
    dec,
    seen_now,
    moved,
    before,
    brown,
    done,
):
    fetch = pltpu.make_async_copy(brown_home, brown, done)
    fetch.start()
    steps, rows, width = brown.shape
    halves = (half_0, half_1, half_2, half_3)
    rests = (rest_0, rest_1, rest_2, rest_3)
    parts = len(halves)
    share = half_0.shape[1]
    hidden = parts * share
    cols = dec.shape[1]
    seen = obs.shape[0]
    first, last_row = packed[:rows, :], packed[rows : rows + 3, :]
    b_out, prior, diff = last_row[0:1], last_row[1:2], last_row[2:3]
    step, lens = vectors[0:1, :], vectors[1:2, :]
    dec[...] = dec_home[...].astype(BF16)

    core = place[0]

    def unpack(ins, outs):
        for q in range(parts):
            block = slice(q * share, (q + 1) * share)
            w_in[q] = ins[q][:width, :]
            w_out[block, :] = outs[q][:width, :]
            w_in_t[block, :] = jnp.transpose(ins[q][:width, :])
            w_out_t[q] = jnp.transpose(outs[q][:width, :])

    pl.when(core == 0)(lambda: unpack(halves, rests))
    pl.when(core == 1)(lambda: unpack(rests, halves))
    for q in range(parts):
        b_in[:, q * share : (q + 1) * share] = halves[q][width:, :].astype(F32)[:1]

    step_b = column(step, rows)
    root_b = jnp.sqrt(step_b)
    lens_b = column(lens, rows)
    inv = 1.0 / diff
    for j in range(seen):
        obs_at[j] = column(vectors[2 + j : 3 + j, :], rows)
    dec_t = jnp.transpose(dec[...])
    w_in_t[hidden : hidden + cols, :] = dec_t
    w_in_t[hidden + cols : hidden + 2 * cols, :] = dec_t

    state[...] = first
    kl_acc[...] = jnp.zeros_like(kl_acc)
    sq_acc[...] = jnp.zeros_like(sq_acc)
    in_acc[...] = jnp.zeros_like(in_acc)
    out_acc[...] = jnp.zeros_like(out_acc)
    acc[...] = jnp.zeros_like(acc)
    acc_dec[...] = jnp.zeros_like(acc_dec)

    early = 4
    seen_now[...] = jnp.zeros_like(seen_now)
    moved[...] = jnp.broadcast_to(-b_out, (rows, width))
    before[...] = jnp.zeros_like(before)

    def observe_some(k, which, total, squares):
        stamp = k.astype(F32)
        product = seen_now[...]
        for j in which:
            misfit = jnp.where(obs_at[j] == stamp, product - obs[j].astype(F32), 0.0)
            squares = squares + misfit * misfit
            total = total + misfit.astype(BF16).astype(F32)
        return total, squares

    def store_back(total, at):
        high = total.astype(BF16)
        seen_back[at, :, :cols] = high
        seen_back[at, :, cols:] = (total - high.astype(F32)).astype(BF16)

    def observe(k, at):
        total, squares = observe_some(k, range(seen), jnp.zeros((rows, cols), F32), sq_acc[...])
        sq_acc[...] = squares
        store_back(total, at)

    def settle(k):
        at = jnp.maximum(k, 0)
        factor = wide(jnp.where(k.astype(F32) < lens_b, step_b, 0.0))
        residual = (moved[...] + b_out + prior * before[...]) * inv
        scaled[at] = residual * inv
        spent = factor * (residual * residual)
        kl_acc[...] += spent[:, :rows] + spent[:, rows:]

    def forward(k, _):
        now = state[...]
        low_now = now.astype(BF16)
        low[k] = low_now
        live = k.astype(F32) < lens_b
        factor = wide(jnp.where(live, step_b, 0.0))
        noise = wide(jnp.where(live, root_b, 0.0))
        base = now + (factor * b_out + diff * noise * brown[k].astype(F32))
        past = k - 1
        total, squares = observe_some(
            past, range(early), jnp.zeros((rows, cols), F32), sq_acc[...]
        )
        floor = jnp.min((squares + jnp.abs(total)).reshape(rows // 8, 8, cols), axis=0)
        nothing = wide(jnp.minimum(floor, 0.0))[None]
        for q in range(parts):
            block = slice(q * share, (q + 1) * share)
            pre = jnp.dot(low_now, w_in[q], preferred_element_type=F32)
            if q == 0:
                pre = (pre.reshape(rows // 8, 8, share) + (nothing + b_in[:, block])).reshape(
                    rows, share
                )
            else:
                pre = pre + b_in[:, block]
            act[k, :, block] = jnp.tanh(pre).astype(BF16)
        settle(past)
        total, squares = observe_some(past, range(early, seen), total, squares)
        sq_acc[...] = squares
        store_back(total, jnp.maximum(past, 0))
        seen_now[...] = jnp.dot(low_now, dec[...], preferred_element_type=F32)
        product = jnp.dot(act[k], w_out[...], preferred_element_type=F32)
        moved[...] = product
        before[...] = now
        state[...] = base + factor * product
        return 0

    fetch.wait()
    lax.fori_loop(0, steps, forward, 0)
    settle(jnp.int32(steps - 1))
    observe(jnp.int32(steps - 1), steps - 1)
    last = state[...].astype(BF16)
    low[steps] = last
    seen_now[...] = jnp.dot(last, dec[...], preferred_element_type=F32)
    observe(jnp.int32(steps), steps)

    state[...] = jnp.dot(
        seen_back[steps], w_in_t[hidden:, :], preferred_element_type=F32
    )

    turned = (((0,), (0,)), ((), ()))

    def back_pair(k_low, pg_now, upd_now):
        for slot in (1, 0):
            k = k_low + slot
            cot = state[...]
            factor = wide(jnp.where(k.astype(F32) < lens_b, step_b, 0.0))
            pull = scaled[k]
            update = factor * (cot + pull)
            low_up = update.astype(BF16)
            upd_now[slot] = low_up
            out_acc[...] += jnp.sum(update.reshape(rows // 8, 8, width), axis=0)
            for q in range(parts):
                block = slice(q * share, (q + 1) * share)
                a = act[k, :, block].astype(F32)
                pre = jnp.dot(low_up, w_out_t[q], preferred_element_type=F32) * (1.0 - a * a)
                pg_now[slot, :, block] = pre.astype(BF16)
                in_acc[:, block] += jnp.sum(pre.reshape(rows // 8, 8, share), axis=0)
            pg_now[slot, :, hidden:] = seen_back[k]
            state[...] = (
                cot
                + factor * (prior * pull)
                + jnp.dot(pg_now[slot], w_in_t[...], preferred_element_type=F32)
            )

    def add_grads(k_low, pg_then, upd_then):
        at = pl.ds(k_low, 2)
        right = low[at].reshape(2 * rows, width)
        left = pg_then[...].reshape(2 * rows, hidden + 2 * cols)
        acc[0] += lax.dot_general(left[:, :hidden], right, turned, preferred_element_type=F32)
        acc_dec[...] += lax.dot_general(
            left[:, hidden:], right, turned, preferred_element_type=F32
        )
        acc[1] += lax.dot_general(
            act[at].reshape(2 * rows, hidden),
            upd_then[...].reshape(2 * rows, width),
            turned,
            preferred_element_type=F32,
        )

    pg_b[...] = jnp.zeros_like(pg_b)
    upd_b[...] = jnp.zeros_like(upd_b)

    def backward(i, _):
        k = steps - 4 - 4 * i
        back_pair(k + 2, pg_a, upd_a)
        add_grads(jnp.minimum(k + 4, steps - 2), pg_b, upd_b)
        back_pair(k, pg_b, upd_b)
        add_grads(k + 2, pg_a, upd_a)
        return 0

    lax.fori_loop(0, steps // 4, backward, 0, unroll=2)
    add_grads(0, pg_b, upd_b)
    grad_init[...] = state[...]
    final = acc_dec[...] + lax.dot_general(
        seen_back[steps], low[steps], turned, preferred_element_type=F32
    )
    spot = place[1]
    lanes = share // cols
    blocks, depth, _ = keep.shape
    slots = width * lanes // depth
    deep = width // slots
    members = slots * parts
    tile = slots * 8
    acc_dec[:, :cols] = jnp.transpose(final[:cols, :] + final[cols:, :])
    in_sum = jnp.sum(in_acc[...], axis=0, keepdims=True)
    out_sum = jnp.sum(out_acc[...], axis=0, keepdims=True)
    kl = 0.5 * jnp.sum(jnp.transpose(kl_acc[...]), axis=0, keepdims=True)
    loglik = -0.5 * jnp.sum(jnp.transpose(sq_acc[...]), axis=0, keepdims=True)
    rest = [out_sum[:, p * cols : (p + 1) * cols] for p in range(width // cols)]
    rest = rest + [loglik, kl]
    rest = rest + [jnp.zeros((8 - lanes - len(rest), cols), F32)]
    for half, out in ((core, keep), (1 - core, send)):
        decs = acc_dec[pl.ds(pl.multiple_of(half * tile, 8), tile), :cols]
        out[members : members + tile // depth] = decs.reshape(tile // depth, depth, cols)
        for s in range(parts):
            q = lax.rem(spot + (parts - s), parts)
            at = pl.ds(q * slots, slots)
            for p in range(lanes):
                block = slice(s * share, (s + 1) * share)
                out[at, p * deep : (p + 1) * deep, :] = acc[
                    half, block, p * cols : (p + 1) * cols
                ].reshape(slots, deep, cols)
            aux = [in_sum[:, s * share + p * cols : s * share + (p + 1) * cols] for p in range(lanes)]
            out[blocks - 1, pl.ds(pl.multiple_of(q * 8, 8), 8), :] = jnp.concatenate(
                aux + rest, axis=0
            )

    divisor = width * lens + cols * seen
    elbo[...] = (loglik - kl) / divisor


def solve(operands, halves, rests, place, slots):
    brown, packed, vectors, dec, observed = operands
    rows, width = brown.shape[1:]
    steps = brown.shape[0]
    parts = len(halves)
    share = halves[0].shape[1]
    hidden = parts * share
    seen, _, cols = observed.shape
    vmem = pl.BlockSpec(memory_space=pltpu.VMEM)
    shape = jax.ShapeDtypeStruct
    depth = width // slots * share // cols
    payload = shape((slots * parts + slots * 8 // depth + parts * 8 // depth, depth, cols), F32)
    outs = (
        payload,
        payload,
        shape((1, rows), F32),
        shape((rows, width), F32),
    )
    return pl.pallas_call(
        series_kernel,
        name="series",
        out_shape=outs,
        in_specs=[pl.BlockSpec(memory_space=pltpu.HBM)]
        + [vmem] * (4 + 2 * parts)
        + [pl.BlockSpec(memory_space=pltpu.SMEM)],
        out_specs=(vmem,) * len(outs),
        scratch_shapes=[
            pltpu.VMEM((steps, rows, hidden), BF16),
            pltpu.VMEM((steps + 1, rows, 2 * cols), BF16),
            pltpu.VMEM((steps + 1, rows, width), BF16),
            pltpu.VMEM((2, rows, hidden + 2 * cols), BF16),
            pltpu.VMEM((2, rows, hidden + 2 * cols), BF16),
            pltpu.VMEM((2, rows, width), BF16),
            pltpu.VMEM((2, rows, width), BF16),
            pltpu.VMEM((steps, rows, width), F32),
            pltpu.VMEM((1, hidden), F32),
            pltpu.VMEM((parts, width, share), BF16),
            pltpu.VMEM((hidden, width), BF16),
            pltpu.VMEM((hidden + 2 * cols, width), BF16),
            pltpu.VMEM((parts, width, share), BF16),
            pltpu.VMEM((seen, rows, cols), F32),
            pltpu.VMEM((rows, width), F32),
            pltpu.VMEM((rows, rows), F32),
            pltpu.VMEM((rows, cols), F32),
            pltpu.VMEM((8, hidden), F32),
            pltpu.VMEM((8, width), F32),
            pltpu.VMEM((2, hidden, width), F32),
            pltpu.VMEM((2 * cols, width), F32),
            pltpu.VMEM((width, cols), BF16),
            pltpu.VMEM((rows, cols), F32),
            pltpu.VMEM((rows, width), F32),
            pltpu.VMEM((rows, width), F32),
            pltpu.VMEM((steps, rows, width), BF16),
            pltpu.SemaphoreType.DMA,
        ],
        compiler_params=pltpu.CompilerParams(
            vmem_limit_bytes=50 * 1024 * 1024,
        ),
        cost_estimate=pl.CostEstimate(
            flops=12 * steps * rows * width * hidden,
            bytes_accessed=8 * 1024 * 1024,
            transcendentals=steps * rows * hidden,
        ),
    )(
        *operands,
        *halves,
        *rests,
        place,
    )


def encode_kernel(slots, parts, mine, other, coded):
    depth, cols = mine.shape[1:]
    members = slots * parts
    decs_end = members + slots * 8 // depth
    total = mine[...] + other[...]

    def scaled_part(part):
        peak = jnp.max(jnp.abs(part), axis=1, keepdims=True)
        power = jnp.floor(jnp.log2(jnp.maximum(peak, 1e-30))) + 1.0
        return part * jnp.exp2(14.0 - power), power

    def over_slots(part):
        full = jnp.broadcast_to(part[:, None], (parts, slots, *part.shape[1:]))
        return full.reshape(members, *part.shape[1:])

    def over_parts(part):
        full = jnp.broadcast_to(part[None], (parts, *part.shape))
        return full.reshape(members, *part.shape[1:])

    weights, weights_power = scaled_part(total[:members])
    decs, decs_power = scaled_part(total[members:decs_end].reshape(slots, 8, cols))
    rest, rest_power = scaled_part(total[decs_end:].reshape(parts, 8, cols))
    rest_high = jnp.round(rest)
    rest_low = (rest - rest_high) * 16384.0
    row = lax.broadcasted_iota(jnp.int32, (members, 8, cols), 1)
    rest_low = jnp.where(row == 6, over_slots(jnp.broadcast_to(rest_power, rest.shape)), over_slots(rest_low))
    decs_power = over_parts(jnp.broadcast_to(decs_power, decs.shape))
    rest_high = jnp.where(row == 6, weights_power, jnp.where(row == 7, decs_power, over_slots(rest_high)))
    full = jnp.concatenate([weights, over_parts(decs), rest_high, rest_low], axis=1)
    coded[...] = jnp.round(full).astype(jnp.int32).astype(jnp.int16)


def encode(mine, other, slots, parts):
    depth, cols = mine.shape[1:]
    vmem = pl.BlockSpec(memory_space=pltpu.VMEM)
    return pl.pallas_call(
        functools.partial(encode_kernel, slots, parts),
        name="encode",
        out_shape=jax.ShapeDtypeStruct((slots * parts, depth + 24, cols), jnp.int16),
        in_specs=[vmem, vmem],
        out_specs=vmem,
        compiler_params=pltpu.CompilerParams(vmem_limit_bytes=16 * 1024 * 1024),
    )(mine, other)


def sum_kernel(scale, parts, spread, rest):
    depth = spread.shape[1]
    weights = depth - 8
    values = parts[...].astype(jnp.int32).astype(F32)
    high, low = values[:, depth : depth + 8], values[:, depth + 8 : depth + 16]

    def unit(row):
        return jnp.exp2(row - 14.0) * scale

    main = jnp.sum(values[:, :weights] * unit(high[:, 6:7]), axis=0)
    decs = jnp.sum(values[:, weights:depth] * unit(high[:, 7:8]), axis=0)
    rest[...] = jnp.sum((high + low * (1.0 / 16384.0)) * unit(low[:, 6:7]), axis=0)
    spread[:, :weights] = jnp.broadcast_to(main[None], (spread.shape[0], *main.shape))
    spread[:, weights:] = jnp.broadcast_to(decs[None], (spread.shape[0], *decs.shape))


def sum_parts(parts, slots, scale):
    _, depth, cols = parts.shape
    vmem = pl.BlockSpec(memory_space=pltpu.VMEM)
    return pl.pallas_call(
        functools.partial(sum_kernel, scale),
        name="sum_parts",
        out_shape=(
            jax.ShapeDtypeStruct((slots, depth - 16, cols), F32),
            jax.ShapeDtypeStruct((8, cols), F32),
        ),
        in_specs=[vmem],
        out_specs=(vmem, vmem),
        compiler_params=pltpu.CompilerParams(vmem_limit_bytes=16 * 1024 * 1024),
    )(parts)


def lay_kernel(place, mine, other, w_in, w_out, dec):
    core = place[0]
    slots, depth, cols = mine.shape
    width = w_in.shape[0]
    deep = width // slots

    def lay(low, high):
        for p in range(w_in.shape[1] // cols):
            rows = slice(p * deep, (p + 1) * deep)
            block = slice(p * cols, (p + 1) * cols)
            w_in[block, :] = jnp.transpose(low[:, rows, :].reshape(width, cols))
            w_out[:, block] = high[:, rows, :].reshape(width, cols)
        dec[: slots * 8, :] = low[:, depth - 8 :, :].reshape(slots * 8, cols)
        dec[slots * 8 :, :] = high[:, depth - 8 :, :].reshape(slots * 8, cols)

    pl.when(core == 0)(lambda: lay(mine, other))
    pl.when(core == 1)(lambda: lay(other, mine))


def lay_out(place, mine, other, width, share, cols):
    vmem = pl.BlockSpec(memory_space=pltpu.VMEM)
    shape = jax.ShapeDtypeStruct
    return pl.pallas_call(
        lay_kernel,
        name="lay_out",
        out_shape=(
            shape((width, share), F32),
            shape((share, width), F32),
            shape((width, cols), F32),
        ),
        in_specs=[pl.BlockSpec(memory_space=pltpu.SMEM), vmem, vmem],
        out_specs=(vmem,) * 3,
        compiler_params=pltpu.CompilerParams(vmem_limit_bytes=8 * 1024 * 1024),
    )(place, mine, other)


AXES = ("y", "z", "c", "x")
RING = ("x", "y", "z")


def shifted(array, axis, by):
    count = lax.axis_size(axis)
    return lax.ppermute(array, axis, [(i, (i + by) % count) for i in range(count)])


def on_device(
    init_state,
    brownian,
    step_size,
    lengths,
    obs_steps,
    observed,
    w_in,
    b_in,
    w_out,
    b_out,
    decoder,
    prior_rate,
    diffusion,
):
    width = init_state.shape[1]
    share = w_in.shape[1]
    parts = lax.axis_size("x")
    slots = lax.axis_size("y") * lax.axis_size("z")
    cols = decoder.shape[1]
    core = lax.axis_index("c")
    spot = lax.axis_index("x")

    bias_rows = jnp.broadcast_to(b_in[None], (16, share))
    half = jnp.concatenate([jnp.where(core == 0, w_in, w_out), bias_rows], axis=0)
    halves = [half] + [shifted(half, "x", by) for by in range(1, parts)]
    packed = jnp.concatenate([init_state, b_out[None], prior_rate[None], diffusion[None]], axis=0)
    vectors = jnp.concatenate(
        [step_size[None], lengths.astype(F32)[None], obs_steps.T.astype(F32)], axis=0
    )
    by_slot = jnp.transpose(observed, (1, 0, 2))
    halves[1], packed, vectors, dec, by_slot = lax.optimization_barrier(
        (halves[1], packed, vectors, decoder.astype(F32), by_slot)
    )
    rests = [jnp.where(core == 0, w_out, w_in)] + [shifted(got, "c", 1) for got in halves[1:]]
    place = jnp.stack([core, spot]).astype(jnp.int32)
    keep, send, elbo, grad_init = solve(
        (brownian, packed, vectors, dec, by_slot), halves, rests, place, slots
    )
    scale = 1.0 / (init_state.shape[0] * lax.axis_size(AXES))
    coded = encode(keep, shifted(send, "c", 1), slots, parts)
    received = lax.all_to_all(coded, RING, 0, 0, tiled=True)
    spread, rest = sum_parts(received, slots, scale)
    own = lax.all_to_all(spread, ("y", "z"), 0, 0, tiled=True)
    other = shifted(own, "c", 1)
    grad_w_in, grad_w_out, grad_decoder = lay_out(place, own, other, width, share, cols)
    per = share // cols
    end = per + width // cols
    return (
        elbo.reshape(-1),
        jnp.sum(rest[end : end + 2], axis=1),
        grad_w_in,
        rest[:per].reshape(-1),
        grad_w_out,
        rest[per:end].reshape(-1),
        grad_decoder,
        grad_init,
    )


def solution(mesh):
    torus = Mesh(mesh.devices.reshape(4, 4, 2, mesh.shape["mp"]), AXES)
    return jax.shard_map(
        on_device,
        mesh=torus,
        in_specs=(
            P(AXES, None),
            P(None, AXES, None),
            P(AXES),
            P(AXES),
            P(AXES, None),
            P(AXES, None, None),
            P(None, "x"),
            P("x"),
            P("x", None),
            P(),
            P(),
            P(),
            P(),
        ),
        out_specs=(
            P(AXES),
            P(),
            P(None, "x"),
            P("x"),
            P("x", None),
            P(),
            P(),
            P(AXES, None),
        ),
        check_vma=False,
    )
```

```python
import functools

import jax
import jax.numpy as jnp
from jax import lax
from jax.experimental import pallas as pl
from jax.experimental.pallas import tpu as pltpu
from jax.sharding import Mesh
from jax.sharding import PartitionSpec as P

F32 = jnp.float32
BF16 = jnp.bfloat16


def wide(x):
    return jnp.concatenate([x, x], axis=1)


def column(row, rows):
    return jnp.transpose(jnp.broadcast_to(row, (rows, rows)))


def series_kernel(
    brown_home,
    packed,
    vectors,
    dec_home,
    obs,
    half_0,
    half_1,
    half_2,
    half_3,
    rest_0,
    rest_1,
    rest_2,
    rest_3,
    place,
    keep,
    send,
    elbo,
    grad_init,
    act,
    seen_back,
    low,
    pg_a,
    pg_b,
    upd_a,
    upd_b,
    scaled,
    b_in,
    w_in,
    w_out,
    w_in_t,
    w_out_t,
    obs_at,
    state,
    kl_acc,
    sq_acc,
    in_acc,
    out_acc,
    acc,
    acc_dec,
    dec,
    seen_now,
    moved,
    before,
    brown,
    done,
):
    fetch = pltpu.make_async_copy(brown_home, brown, done)
    fetch.start()
    steps, rows, width = brown.shape
    halves = (half_0, half_1, half_2, half_3)
    rests = (rest_0, rest_1, rest_2, rest_3)
    parts = len(halves)
    share = half_0.shape[1]
    hidden = parts * share
    cols = dec.shape[1]
    seen = obs.shape[0]
    first, last_row = packed[:rows, :], packed[rows : rows + 3, :]
    b_out, prior, diff = last_row[0:1], last_row[1:2], last_row[2:3]
    step, lens = vectors[0:1, :], vectors[1:2, :]
    dec[...] = dec_home[...].astype(BF16)

    core = place[0]

    def unpack(ins, outs):
        for q in range(parts):
            block = slice(q * share, (q + 1) * share)
            w_in[q] = ins[q][:width, :]
            w_out[block, :] = outs[q][:width, :]
            w_in_t[block, :] = jnp.transpose(ins[q][:width, :])
            w_out_t[q] = jnp.transpose(outs[q][:width, :])

    pl.when(core == 0)(lambda: unpack(halves, rests))
    pl.when(core == 1)(lambda: unpack(rests, halves))
    for q in range(parts):
        b_in[:, q * share : (q + 1) * share] = halves[q][width:, :].astype(F32)[:1]

    step_b = column(step, rows)
    root_b = jnp.sqrt(step_b)
    lens_b = column(lens, rows)
    inv = 1.0 / diff
    for j in range(seen):
        obs_at[j] = column(vectors[2 + j : 3 + j, :], rows)
    dec_t = jnp.transpose(dec[...])
    w_in_t[hidden : hidden + cols, :] = dec_t
    w_in_t[hidden + cols : hidden + 2 * cols, :] = dec_t

    state[...] = first
    kl_acc[...] = jnp.zeros_like(kl_acc)
    sq_acc[...] = jnp.zeros_like(sq_acc)
    in_acc[...] = jnp.zeros_like(in_acc)
    out_acc[...] = jnp.zeros_like(out_acc)
    acc[...] = jnp.zeros_like(acc)
    acc_dec[...] = jnp.zeros_like(acc_dec)

    early = 4
    seen_now[...] = jnp.zeros_like(seen_now)
    moved[...] = jnp.broadcast_to(-b_out, (rows, width))
    before[...] = jnp.zeros_like(before)

    def observe_some(k, which, total, squares):
        stamp = k.astype(F32)
        product = seen_now[...]
        for j in which:
            misfit = jnp.where(obs_at[j] == stamp, product - obs[j].astype(F32), 0.0)
            squares = squares + misfit * misfit
            total = total + misfit.astype(BF16).astype(F32)
        return total, squares

    def store_back(total, at):
        high = total.astype(BF16)
        seen_back[at, :, :cols] = high
        seen_back[at, :, cols:] = (total - high.astype(F32)).astype(BF16)

    def observe(k, at):
        total, squares = observe_some(k, range(seen), jnp.zeros((rows, cols), F32), sq_acc[...])
        sq_acc[...] = squares
        store_back(total, at)

    def settle(k):
        at = jnp.maximum(k, 0)
        factor = wide(jnp.where(k.astype(F32) < lens_b, step_b, 0.0))
        residual = (moved[...] + b_out + prior * before[...]) * inv
        scaled[at] = residual * inv
        spent = factor * (residual * residual)
        kl_acc[...] += spent[:, :rows] + spent[:, rows:]

    def forward(k, _):
        now = state[...]
        low_now = now.astype(BF16)
        low[k] = low_now
        live = k.astype(F32) < lens_b
        factor = wide(jnp.where(live, step_b, 0.0))
        noise = wide(jnp.where(live, root_b, 0.0))
        base = now + (factor * b_out + diff * noise * brown[k].astype(F32))
        past = k - 1
        total, squares = observe_some(
            past, range(early), jnp.zeros((rows, cols), F32), sq_acc[...]
        )
        floor = jnp.min((squares + jnp.abs(total)).reshape(rows // 8, 8, cols), axis=0)
        nothing = wide(jnp.minimum(floor, 0.0))[None]
        for q in range(parts):
            block = slice(q * share, (q + 1) * share)
            pre = jnp.dot(low_now, w_in[q], preferred_element_type=F32)
            if q == 0:
                pre = (pre.reshape(rows // 8, 8, share) + (nothing + b_in[:, block])).reshape(
                    rows, share
                )
            else:
                pre = pre + b_in[:, block]
            act[k, :, block] = jnp.tanh(pre).astype(BF16)
        settle(past)
        total, squares = observe_some(past, range(early, seen), total, squares)
        sq_acc[...] = squares
        store_back(total, jnp.maximum(past, 0))
        seen_now[...] = jnp.dot(low_now, dec[...], preferred_element_type=F32)
        product = jnp.dot(act[k], w_out[...], preferred_element_type=F32)
        moved[...] = product
        before[...] = now
        state[...] = base + factor * product
        return 0

    fetch.wait()
    lax.fori_loop(0, steps, forward, 0)
    settle(jnp.int32(steps - 1))
    observe(jnp.int32(steps - 1), steps - 1)
    last = state[...].astype(BF16)
    low[steps] = last
    seen_now[...] = jnp.dot(last, dec[...], preferred_element_type=F32)
    observe(jnp.int32(steps), steps)

    state[...] = jnp.dot(
        seen_back[steps], w_in_t[hidden:, :], preferred_element_type=F32
    )

    turned = (((0,), (0,)), ((), ()))

    def back_pair(k_low, pg_now, upd_now):
        for slot in (1, 0):
            k = k_low + slot
            cot = state[...]
            factor = wide(jnp.where(k.astype(F32) < lens_b, step_b, 0.0))
            pull = scaled[k]
            update = factor * (cot + pull)
            low_up = update.astype(BF16)
            upd_now[slot] = low_up
            out_acc[...] += jnp.sum(update.reshape(rows // 8, 8, width), axis=0)
            for q in range(parts):
                block = slice(q * share, (q + 1) * share)
                a = act[k, :, block].astype(F32)
                pre = jnp.dot(low_up, w_out_t[q], preferred_element_type=F32) * (1.0 - a * a)
                pg_now[slot, :, block] = pre.astype(BF16)
                in_acc[:, block] += jnp.sum(pre.reshape(rows // 8, 8, share), axis=0)
            pg_now[slot, :, hidden:] = seen_back[k]
            state[...] = (
                cot
                + factor * (prior * pull)
                + jnp.dot(pg_now[slot], w_in_t[...], preferred_element_type=F32)
            )

    def add_grads(k_low, pg_then, upd_then):
        at = pl.ds(k_low, 2)
        right = low[at].reshape(2 * rows, width)
        left = pg_then[...].reshape(2 * rows, hidden + 2 * cols)
        acc[0] += lax.dot_general(left[:, :hidden], right, turned, preferred_element_type=F32)
        acc_dec[...] += lax.dot_general(
            left[:, hidden:], right, turned, preferred_element_type=F32
        )
        acc[1] += lax.dot_general(
            act[at].reshape(2 * rows, hidden),
            upd_then[...].reshape(2 * rows, width),
            turned,
            preferred_element_type=F32,
        )

    pg_b[...] = jnp.zeros_like(pg_b)
    upd_b[...] = jnp.zeros_like(upd_b)

    def backward(i, _):
        k = steps - 4 - 4 * i
        back_pair(k + 2, pg_a, upd_a)
        add_grads(jnp.minimum(k + 4, steps - 2), pg_b, upd_b)
        back_pair(k, pg_b, upd_b)
        add_grads(k + 2, pg_a, upd_a)
        return 0

    lax.fori_loop(0, steps // 4, backward, 0, unroll=4)
    add_grads(0, pg_b, upd_b)
    grad_init[...] = state[...]
    final = acc_dec[...] + lax.dot_general(
        seen_back[steps], low[steps], turned, preferred_element_type=F32
    )
    spot = place[1]
    lanes = share // cols
    blocks, depth, _ = keep.shape
    slots = width * lanes // depth
    deep = width // slots
    members = slots * parts
    tile = slots * 8
    acc_dec[:, :cols] = jnp.transpose(final[:cols, :] + final[cols:, :])
    in_sum = jnp.sum(in_acc[...], axis=0, keepdims=True)
    out_sum = jnp.sum(out_acc[...], axis=0, keepdims=True)
    kl = 0.5 * jnp.sum(jnp.transpose(kl_acc[...]), axis=0, keepdims=True)
    loglik = -0.5 * jnp.sum(jnp.transpose(sq_acc[...]), axis=0, keepdims=True)
    rest = [out_sum[:, p * cols : (p + 1) * cols] for p in range(width // cols)]
    rest = rest + [loglik, kl]
    rest = rest + [jnp.zeros((8 - lanes - len(rest), cols), F32)]
    for half, out in ((core, keep), (1 - core, send)):
        decs = acc_dec[pl.ds(pl.multiple_of(half * tile, 8), tile), :cols]
        out[members : members + tile // depth] = decs.reshape(tile // depth, depth, cols)
        for s in range(parts):
            q = lax.rem(spot + (parts - s), parts)
            at = pl.ds(q * slots, slots)
            for p in range(lanes):
                block = slice(s * share, (s + 1) * share)
                out[at, p * deep : (p + 1) * deep, :] = acc[
                    half, block, p * cols : (p + 1) * cols
                ].reshape(slots, deep, cols)
            aux = [in_sum[:, s * share + p * cols : s * share + (p + 1) * cols] for p in range(lanes)]
            out[blocks - 1, pl.ds(pl.multiple_of(q * 8, 8), 8), :] = jnp.concatenate(
                aux + rest, axis=0
            )

    divisor = width * lens + cols * seen
    elbo[...] = (loglik - kl) / divisor


def solve(operands, halves, rests, place, slots):
    brown, packed, vectors, dec, observed = operands
    rows, width = brown.shape[1:]
    steps = brown.shape[0]
    parts = len(halves)
    share = halves[0].shape[1]
    hidden = parts * share
    seen, _, cols = observed.shape
    vmem = pl.BlockSpec(memory_space=pltpu.VMEM)
    shape = jax.ShapeDtypeStruct
    depth = width // slots * share // cols
    payload = shape((slots * parts + slots * 8 // depth + parts * 8 // depth, depth, cols), F32)
    outs = (
        payload,
        payload,
        shape((1, rows), F32),
        shape((rows, width), F32),
    )
    return pl.pallas_call(
        series_kernel,
        name="series",
        out_shape=outs,
        in_specs=[pl.BlockSpec(memory_space=pltpu.HBM)]
        + [vmem] * (4 + 2 * parts)
        + [pl.BlockSpec(memory_space=pltpu.SMEM)],
        out_specs=(vmem,) * len(outs),
        scratch_shapes=[
            pltpu.VMEM((steps, rows, hidden), BF16),
            pltpu.VMEM((steps + 1, rows, 2 * cols), BF16),
            pltpu.VMEM((steps + 1, rows, width), BF16),
            pltpu.VMEM((2, rows, hidden + 2 * cols), BF16),
            pltpu.VMEM((2, rows, hidden + 2 * cols), BF16),
            pltpu.VMEM((2, rows, width), BF16),
            pltpu.VMEM((2, rows, width), BF16),
            pltpu.VMEM((steps, rows, width), F32),
            pltpu.VMEM((1, hidden), F32),
            pltpu.VMEM((parts, width, share), BF16),
            pltpu.VMEM((hidden, width), BF16),
            pltpu.VMEM((hidden + 2 * cols, width), BF16),
            pltpu.VMEM((parts, width, share), BF16),
            pltpu.VMEM((seen, rows, cols), F32),
            pltpu.VMEM((rows, width), F32),
            pltpu.VMEM((rows, rows), F32),
            pltpu.VMEM((rows, cols), F32),
            pltpu.VMEM((8, hidden), F32),
            pltpu.VMEM((8, width), F32),
            pltpu.VMEM((2, hidden, width), F32),
            pltpu.VMEM((2 * cols, width), F32),
            pltpu.VMEM((width, cols), BF16),
            pltpu.VMEM((rows, cols), F32),
            pltpu.VMEM((rows, width), F32),
            pltpu.VMEM((rows, width), F32),
            pltpu.VMEM((steps, rows, width), BF16),
            pltpu.SemaphoreType.DMA,
        ],
        compiler_params=pltpu.CompilerParams(
            vmem_limit_bytes=50 * 1024 * 1024,
        ),
        cost_estimate=pl.CostEstimate(
            flops=12 * steps * rows * width * hidden,
            bytes_accessed=8 * 1024 * 1024,
            transcendentals=steps * rows * hidden,
        ),
    )(
        *operands,
        *halves,
        *rests,
        place,
    )


def encode_kernel(slots, parts, mine, other, coded):
    depth, cols = mine.shape[1:]
    members = slots * parts
    decs_end = members + slots * 8 // depth
    total = mine[...] + other[...]

    def scaled_part(part):
        peak = jnp.max(jnp.abs(part), axis=1, keepdims=True)
        power = jnp.floor(jnp.log2(jnp.maximum(peak, 1e-30))) + 1.0
        return part * jnp.exp2(14.0 - power), power

    def over_slots(part):
        full = jnp.broadcast_to(part[:, None], (parts, slots, *part.shape[1:]))
        return full.reshape(members, *part.shape[1:])

    def over_parts(part):
        full = jnp.broadcast_to(part[None], (parts, *part.shape))
        return full.reshape(members, *part.shape[1:])

    weights, weights_power = scaled_part(total[:members])
    decs, decs_power = scaled_part(total[members:decs_end].reshape(slots, 8, cols))
    rest, rest_power = scaled_part(total[decs_end:].reshape(parts, 8, cols))
    rest_high = jnp.round(rest)
    rest_low = (rest - rest_high) * 16384.0
    row = lax.broadcasted_iota(jnp.int32, (members, 8, cols), 1)
    rest_low = jnp.where(row == 6, over_slots(jnp.broadcast_to(rest_power, rest.shape)), over_slots(rest_low))
    decs_power = over_parts(jnp.broadcast_to(decs_power, decs.shape))
    rest_high = jnp.where(row == 6, weights_power, jnp.where(row == 7, decs_power, over_slots(rest_high)))
    full = jnp.concatenate([weights, over_parts(decs), rest_high, rest_low], axis=1)
    coded[...] = jnp.round(full).astype(jnp.int32).astype(jnp.int16)


def encode(mine, other, slots, parts):
    depth, cols = mine.shape[1:]
    vmem = pl.BlockSpec(memory_space=pltpu.VMEM)
    return pl.pallas_call(
        functools.partial(encode_kernel, slots, parts),
        name="encode",
        out_shape=jax.ShapeDtypeStruct((slots * parts, depth + 24, cols), jnp.int16),
        in_specs=[vmem, vmem],
        out_specs=vmem,
        compiler_params=pltpu.CompilerParams(vmem_limit_bytes=16 * 1024 * 1024),
    )(mine, other)


def sum_kernel(scale, parts, spread, rest):
    depth = spread.shape[1]
    weights = depth - 8
    values = parts[...].astype(jnp.int32).astype(F32)
    high, low = values[:, depth : depth + 8], values[:, depth + 8 : depth + 16]

    def unit(row):
        return jnp.exp2(row - 14.0) * scale

    main = jnp.sum(values[:, :weights] * unit(high[:, 6:7]), axis=0)
    decs = jnp.sum(values[:, weights:depth] * unit(high[:, 7:8]), axis=0)
    rest[...] = jnp.sum((high + low * (1.0 / 16384.0)) * unit(low[:, 6:7]), axis=0)
    spread[:, :weights] = jnp.broadcast_to(main[None], (spread.shape[0], *main.shape))
    spread[:, weights:] = jnp.broadcast_to(decs[None], (spread.shape[0], *decs.shape))


def sum_parts(parts, slots, scale):
    _, depth, cols = parts.shape
    vmem = pl.BlockSpec(memory_space=pltpu.VMEM)
    return pl.pallas_call(
        functools.partial(sum_kernel, scale),
        name="sum_parts",
        out_shape=(
            jax.ShapeDtypeStruct((slots, depth - 16, cols), F32),
            jax.ShapeDtypeStruct((8, cols), F32),
        ),
        in_specs=[vmem],
        out_specs=(vmem, vmem),
        compiler_params=pltpu.CompilerParams(vmem_limit_bytes=16 * 1024 * 1024),
    )(parts)


def lay_kernel(place, mine, other, w_in, w_out, dec):
    core = place[0]
    slots, depth, cols = mine.shape
    width = w_in.shape[0]
    deep = width // slots

    def lay(low, high):
        for p in range(w_in.shape[1] // cols):
            rows = slice(p * deep, (p + 1) * deep)
            block = slice(p * cols, (p + 1) * cols)
            w_in[block, :] = jnp.transpose(low[:, rows, :].reshape(width, cols))
            w_out[:, block] = high[:, rows, :].reshape(width, cols)
        dec[: slots * 8, :] = low[:, depth - 8 :, :].reshape(slots * 8, cols)
        dec[slots * 8 :, :] = high[:, depth - 8 :, :].reshape(slots * 8, cols)

    pl.when(core == 0)(lambda: lay(mine, other))
    pl.when(core == 1)(lambda: lay(other, mine))


def lay_out(place, mine, other, width, share, cols):
    vmem = pl.BlockSpec(memory_space=pltpu.VMEM)
    shape = jax.ShapeDtypeStruct
    return pl.pallas_call(
        lay_kernel,
        name="lay_out",
        out_shape=(
            shape((width, share), F32),
            shape((share, width), F32),
            shape((width, cols), F32),
        ),
        in_specs=[pl.BlockSpec(memory_space=pltpu.SMEM), vmem, vmem],
        out_specs=(vmem,) * 3,
        compiler_params=pltpu.CompilerParams(vmem_limit_bytes=8 * 1024 * 1024),
    )(place, mine, other)


AXES = ("y", "z", "c", "x")
RING = ("x", "y", "z")


def shifted(array, axis, by):
    count = lax.axis_size(axis)
    return lax.ppermute(array, axis, [(i, (i + by) % count) for i in range(count)])


def on_device(
    init_state,
    brownian,
    step_size,
    lengths,
    obs_steps,
    observed,
    w_in,
    b_in,
    w_out,
    b_out,
    decoder,
    prior_rate,
    diffusion,
):
    width = init_state.shape[1]
    share = w_in.shape[1]
    parts = lax.axis_size("x")
    slots = lax.axis_size("y") * lax.axis_size("z")
    cols = decoder.shape[1]
    core = lax.axis_index("c")
    spot = lax.axis_index("x")

    tall = ((0, 16), (0, 0))
    row = lax.broadcasted_iota(jnp.int32, (width + 16, share), 0)
    own = jnp.where(core == 0, jnp.pad(w_in, tall), jnp.pad(w_out, tall))
    half = jnp.where(row < width, own, b_in[None])
    halves = [half] + [shifted(half, "x", by) for by in range(1, parts)]
    packed = jnp.concatenate([init_state, b_out[None], prior_rate[None], diffusion[None]], axis=0)
    vectors = jnp.concatenate(
        [step_size[None], lengths.astype(F32)[None], obs_steps.T.astype(F32)], axis=0
    )
    by_slot = jnp.transpose(observed, (1, 0, 2))
    _, w_in, w_out = lax.optimization_barrier((half, w_in, w_out))
    rest = jnp.where(core == 0, w_out, w_in)
    halves[1], packed, vectors, dec, by_slot, rest = lax.optimization_barrier(
        (halves[1], packed, vectors, decoder.astype(F32), by_slot, rest)
    )
    rests = [rest] + [shifted(got, "c", 1) for got in halves[1:]]
    place = jnp.stack([core, spot]).astype(jnp.int32)
    keep, send, elbo, grad_init = solve(
        (brownian, packed, vectors, dec, by_slot), halves, rests, place, slots
    )
    scale = 1.0 / (init_state.shape[0] * lax.axis_size(AXES))
    coded = encode(keep, shifted(send, "c", 1), slots, parts)
    received = lax.all_to_all(coded, RING, 0, 0, tiled=True)
    spread, rest = sum_parts(received, slots, scale)
    own = lax.all_to_all(spread, ("y", "z"), 0, 0, tiled=True)
    other = shifted(own, "c", 1)
    grad_w_in, grad_w_out, grad_decoder = lay_out(place, own, other, width, share, cols)
    per = share // cols
    end = per + width // cols
    return (
        elbo.reshape(-1),
        jnp.sum(rest[end : end + 2], axis=1),
        grad_w_in,
        rest[:per].reshape(-1),
        grad_w_out,
        rest[per:end].reshape(-1),
        grad_decoder,
        grad_init,
    )


def solution(mesh):
    torus = Mesh(mesh.devices.reshape(4, 4, 2, mesh.shape["mp"]), AXES)
    return jax.shard_map(
        on_device,
        mesh=torus,
        in_specs=(
            P(AXES, None),
            P(None, AXES, None),
            P(AXES),
            P(AXES),
            P(AXES, None),
            P(AXES, None, None),
            P(None, "x"),
            P("x"),
            P("x", None),
            P(),
            P(),
            P(),
            P(),
        ),
        out_specs=(
            P(AXES),
            P(),
            P(None, "x"),
            P("x"),
            P("x", None),
            P(),
            P(),
            P(AXES, None),
        ),
        check_vma=False,
    )
```

```python
import functools

import jax
import jax.numpy as jnp
from jax import lax
from jax.experimental import pallas as pl
from jax.experimental.pallas import tpu as pltpu
from jax.sharding import Mesh
from jax.sharding import PartitionSpec as P

F32 = jnp.float32
BF16 = jnp.bfloat16


def wide(x):
    return jnp.concatenate([x, x], axis=1)


def column(row, rows):
    return jnp.transpose(jnp.broadcast_to(row, (rows, rows)))


def series_kernel(
    brown_home,
    packed,
    vectors,
    dec_home,
    obs,
    half_0,
    half_1,
    half_2,
    half_3,
    rest_0,
    rest_1,
    rest_2,
    rest_3,
    place,
    keep,
    send,
    elbo,
    grad_init,
    act,
    seen_back,
    low,
    pg_a,
    pg_b,
    upd_a,
    upd_b,
    scaled,
    b_in,
    w_in,
    w_out,
    w_in_t,
    w_out_t,
    obs_at,
    state,
    kl_acc,
    sq_acc,
    in_acc,
    out_acc,
    acc,
    acc_dec,
    dec,
    seen_now,
    moved,
    before,
    brown,
    done,
):
    fetch = pltpu.make_async_copy(brown_home, brown, done)
    fetch.start()
    steps, rows, width = brown.shape
    halves = (half_0, half_1, half_2, half_3)
    rests = (rest_0, rest_1, rest_2, rest_3)
    parts = len(halves)
    share = half_0.shape[1]
    hidden = parts * share
    cols = dec.shape[1]
    seen = obs.shape[0]
    first, last_row = packed[:rows, :], packed[rows : rows + 3, :]
    b_out, prior, diff = last_row[0:1], last_row[1:2], last_row[2:3]
    step, lens = vectors[0:1, :], vectors[1:2, :]
    dec[...] = dec_home[...].astype(BF16)

    core = place[0]

    def unpack(ins, outs):
        for q in range(parts):
            block = slice(q * share, (q + 1) * share)
            w_in[q] = ins[q][:width, :]
            w_out[block, :] = outs[q][:width, :]
            w_in_t[block, :] = jnp.transpose(ins[q][:width, :])
            w_out_t[q] = jnp.transpose(outs[q][:width, :])

    pl.when(core == 0)(lambda: unpack(halves, rests))
    pl.when(core == 1)(lambda: unpack(rests, halves))
    for q in range(parts):
        b_in[:, q * share : (q + 1) * share] = halves[q][width:, :].astype(F32)[:1]

    step_b = column(step, rows)
    root_b = jnp.sqrt(step_b)
    lens_b = column(lens, rows)
    inv = 1.0 / diff
    for j in range(seen):
        obs_at[j] = column(vectors[2 + j : 3 + j, :], rows)
    dec_t = jnp.transpose(dec[...])
    w_in_t[hidden : hidden + cols, :] = dec_t
    w_in_t[hidden + cols : hidden + 2 * cols, :] = dec_t

    state[...] = first
    kl_acc[...] = jnp.zeros_like(kl_acc)
    sq_acc[...] = jnp.zeros_like(sq_acc)
    in_acc[...] = jnp.zeros_like(in_acc)
    out_acc[...] = jnp.zeros_like(out_acc)
    acc[...] = jnp.zeros_like(acc)
    acc_dec[...] = jnp.zeros_like(acc_dec)

    early = 4
    seen_now[...] = jnp.zeros_like(seen_now)
    moved[...] = jnp.broadcast_to(-b_out, (rows, width))
    before[...] = jnp.zeros_like(before)

    def observe_some(k, which, total, squares):
        stamp = k.astype(F32)
        product = seen_now[...]
        for j in which:
            misfit = jnp.where(obs_at[j] == stamp, product - obs[j].astype(F32), 0.0)
            squares = squares + misfit * misfit
            total = total + misfit.astype(BF16).astype(F32)
        return total, squares

    def store_back(total, at):
        high = total.astype(BF16)
        seen_back[at, :, :cols] = high
        seen_back[at, :, cols:] = (total - high.astype(F32)).astype(BF16)

    def observe(k, at):
        total, squares = observe_some(k, range(seen), jnp.zeros((rows, cols), F32), sq_acc[...])
        sq_acc[...] = squares
        store_back(total, at)

    def settle(k):
        at = jnp.maximum(k, 0)
        factor = wide(jnp.where(k.astype(F32) < lens_b, step_b, 0.0))
        residual = (moved[...] + b_out + prior * before[...]) * inv
        scaled[at] = residual * inv
        spent = factor * (residual * residual)
        kl_acc[...] += spent[:, :rows] + spent[:, rows:]

    def forward(k, _):
        now = state[...]
        low_now = now.astype(BF16)
        low[k] = low_now
        live = k.astype(F32) < lens_b
        factor = wide(jnp.where(live, step_b, 0.0))
        noise = wide(jnp.where(live, root_b, 0.0))
        base = now + (factor * b_out + diff * noise * brown[k].astype(F32))
        past = k - 1
        total, squares = observe_some(
            past, range(early), jnp.zeros((rows, cols), F32), sq_acc[...]
        )
        floor = jnp.min((squares + jnp.abs(total)).reshape(rows // 8, 8, cols), axis=0)
        nothing = wide(jnp.minimum(floor, 0.0))[None]
        for q in range(parts):
            block = slice(q * share, (q + 1) * share)
            pre = jnp.dot(low_now, w_in[q], preferred_element_type=F32)
            if q == 0:
                pre = (pre.reshape(rows // 8, 8, share) + (nothing + b_in[:, block])).reshape(
                    rows, share
                )
            else:
                pre = pre + b_in[:, block]
            act[k, :, block] = jnp.tanh(pre).astype(BF16)
        settle(past)
        total, squares = observe_some(past, range(early, seen), total, squares)
        sq_acc[...] = squares
        store_back(total, jnp.maximum(past, 0))
        seen_now[...] = jnp.dot(low_now, dec[...], preferred_element_type=F32)
        product = jnp.dot(act[k], w_out[...], preferred_element_type=F32)
        moved[...] = product
        before[...] = now
        state[...] = base + factor * product
        return 0

    fetch.wait()
    lax.fori_loop(0, steps, forward, 0)
    settle(jnp.int32(steps - 1))
    observe(jnp.int32(steps - 1), steps - 1)
    last = state[...].astype(BF16)
    low[steps] = last
    seen_now[...] = jnp.dot(last, dec[...], preferred_element_type=F32)
    observe(jnp.int32(steps), steps)

    state[...] = jnp.dot(
        seen_back[steps], w_in_t[hidden:, :], preferred_element_type=F32
    )

    turned = (((0,), (0,)), ((), ()))

    def back_pair(k_low, pg_now, upd_now):
        for slot in (1, 0):
            k = k_low + slot
            cot = state[...]
            factor = wide(jnp.where(k.astype(F32) < lens_b, step_b, 0.0))
            pull = scaled[k]
            update = factor * (cot + pull)
            low_up = update.astype(BF16)
            upd_now[slot] = low_up
            out_acc[...] += jnp.sum(update.reshape(rows // 8, 8, width), axis=0)
            for q in range(parts):
                block = slice(q * share, (q + 1) * share)
                a = act[k, :, block].astype(F32)
                pre = jnp.dot(low_up, w_out_t[q], preferred_element_type=F32) * (1.0 - a * a)
                pg_now[slot, :, block] = pre.astype(BF16)
                in_acc[:, block] += jnp.sum(pre.reshape(rows // 8, 8, share), axis=0)
            pg_now[slot, :, hidden:] = seen_back[k]
            state[...] = (
                cot
                + factor * (prior * pull)
                + jnp.dot(pg_now[slot], w_in_t[...], preferred_element_type=F32)
            )

    def add_grads(k_low, pg_then, upd_then):
        at = pl.ds(k_low, 2)
        right = low[at].reshape(2 * rows, width)
        left = pg_then[...].reshape(2 * rows, hidden + 2 * cols)
        acc[0] += lax.dot_general(left[:, :hidden], right, turned, preferred_element_type=F32)
        acc_dec[...] += lax.dot_general(
            left[:, hidden:], right, turned, preferred_element_type=F32
        )
        acc[1] += lax.dot_general(
            act[at].reshape(2 * rows, hidden),
            upd_then[...].reshape(2 * rows, width),
            turned,
            preferred_element_type=F32,
        )

    pg_b[...] = jnp.zeros_like(pg_b)
    upd_b[...] = jnp.zeros_like(upd_b)

    def backward(i, _):
        k = steps - 4 - 4 * i
        back_pair(k + 2, pg_a, upd_a)
        add_grads(jnp.minimum(k + 4, steps - 2), pg_b, upd_b)
        back_pair(k, pg_b, upd_b)
        add_grads(k + 2, pg_a, upd_a)
        return 0

    lax.fori_loop(0, steps // 4, backward, 0, unroll=4)
    add_grads(0, pg_b, upd_b)
    grad_init[...] = state[...]
    final = acc_dec[...] + lax.dot_general(
        seen_back[steps], low[steps], turned, preferred_element_type=F32
    )
    spot = place[1]
    lanes = share // cols
    blocks, depth, _ = keep.shape
    slots = width * lanes // depth
    deep = width // slots
    members = slots * parts
    tile = slots * 8
    acc_dec[:, :cols] = jnp.transpose(final[:cols, :] + final[cols:, :])
    in_sum = jnp.sum(in_acc[...], axis=0, keepdims=True)
    out_sum = jnp.sum(out_acc[...], axis=0, keepdims=True)
    kl = 0.5 * jnp.sum(jnp.transpose(kl_acc[...]), axis=0, keepdims=True)
    loglik = -0.5 * jnp.sum(jnp.transpose(sq_acc[...]), axis=0, keepdims=True)
    rest = [out_sum[:, p * cols : (p + 1) * cols] for p in range(width // cols)]
    rest = rest + [loglik, kl]
    rest = rest + [jnp.zeros((8 - lanes - len(rest), cols), F32)]
    for half, out in ((core, keep), (1 - core, send)):
        decs = acc_dec[pl.ds(pl.multiple_of(half * tile, 8), tile), :cols]
        out[members : members + tile // depth] = decs.reshape(tile // depth, depth, cols)
        for s in range(parts):
            q = lax.rem(spot + (parts - s), parts)
            at = pl.ds(q * slots, slots)
            for p in range(lanes):
                block = slice(s * share, (s + 1) * share)
                out[at, p * deep : (p + 1) * deep, :] = acc[
                    half, block, p * cols : (p + 1) * cols
                ].reshape(slots, deep, cols)
            aux = [in_sum[:, s * share + p * cols : s * share + (p + 1) * cols] for p in range(lanes)]
            out[blocks - 1, pl.ds(pl.multiple_of(q * 8, 8), 8), :] = jnp.concatenate(
                aux + rest, axis=0
            )

    divisor = width * lens + cols * seen
    elbo[...] = (loglik - kl) / divisor


def solve(operands, halves, rests, place, slots):
    brown, packed, vectors, dec, observed = operands
    rows, width = brown.shape[1:]
    steps = brown.shape[0]
    parts = len(halves)
    share = halves[0].shape[1]
    hidden = parts * share
    seen, _, cols = observed.shape
    vmem = pl.BlockSpec(memory_space=pltpu.VMEM)
    shape = jax.ShapeDtypeStruct
    depth = width // slots * share // cols
    payload = shape((slots * parts + slots * 8 // depth + parts * 8 // depth, depth, cols), F32)
    outs = (
        payload,
        payload,
        shape((1, rows), F32),
        shape((rows, width), F32),
    )
    return pl.pallas_call(
        series_kernel,
        name="series",
        out_shape=outs,
        in_specs=[pl.BlockSpec(memory_space=pltpu.HBM)]
        + [vmem] * (4 + 2 * parts)
        + [pl.BlockSpec(memory_space=pltpu.SMEM)],
        out_specs=(vmem,) * len(outs),
        scratch_shapes=[
            pltpu.VMEM((steps, rows, hidden), BF16),
            pltpu.VMEM((steps + 1, rows, 2 * cols), BF16),
            pltpu.VMEM((steps + 1, rows, width), BF16),
            pltpu.VMEM((2, rows, hidden + 2 * cols), BF16),
            pltpu.VMEM((2, rows, hidden + 2 * cols), BF16),
            pltpu.VMEM((2, rows, width), BF16),
            pltpu.VMEM((2, rows, width), BF16),
            pltpu.VMEM((steps, rows, width), F32),
            pltpu.VMEM((1, hidden), F32),
            pltpu.VMEM((parts, width, share), BF16),
            pltpu.VMEM((hidden, width), BF16),
            pltpu.VMEM((hidden + 2 * cols, width), BF16),
            pltpu.VMEM((parts, width, share), BF16),
            pltpu.VMEM((seen, rows, cols), F32),
            pltpu.VMEM((rows, width), F32),
            pltpu.VMEM((rows, rows), F32),
            pltpu.VMEM((rows, cols), F32),
            pltpu.VMEM((8, hidden), F32),
            pltpu.VMEM((8, width), F32),
            pltpu.VMEM((2, hidden, width), F32),
            pltpu.VMEM((2 * cols, width), F32),
            pltpu.VMEM((width, cols), BF16),
            pltpu.VMEM((rows, cols), F32),
            pltpu.VMEM((rows, width), F32),
            pltpu.VMEM((rows, width), F32),
            pltpu.VMEM((steps, rows, width), BF16),
            pltpu.SemaphoreType.DMA,
        ],
        compiler_params=pltpu.CompilerParams(
            vmem_limit_bytes=50 * 1024 * 1024,
        ),
        cost_estimate=pl.CostEstimate(
            flops=12 * steps * rows * width * hidden,
            bytes_accessed=8 * 1024 * 1024,
            transcendentals=steps * rows * hidden,
        ),
    )(
        *operands,
        *halves,
        *rests,
        place,
    )


def encode_kernel(slots, parts, mine, other, coded):
    depth, cols = mine.shape[1:]
    members = slots * parts
    decs_end = members + slots * 8 // depth
    total = mine[...] + other[...]

    def scaled_part(part):
        peak = jnp.max(jnp.abs(part), axis=1, keepdims=True)
        power = jnp.floor(jnp.log2(jnp.maximum(peak, 1e-30))) + 1.0
        return part * jnp.exp2(14.0 - power), power

    def over_slots(part):
        full = jnp.broadcast_to(part[:, None], (parts, slots, *part.shape[1:]))
        return full.reshape(members, *part.shape[1:])

    def over_parts(part):
        full = jnp.broadcast_to(part[None], (parts, *part.shape))
        return full.reshape(members, *part.shape[1:])

    weights, weights_power = scaled_part(total[:members])
    decs, decs_power = scaled_part(total[members:decs_end].reshape(slots, 8, cols))
    rest, rest_power = scaled_part(total[decs_end:].reshape(parts, 8, cols))
    rest_high = jnp.round(rest)
    rest_low = (rest - rest_high) * 16384.0
    row = lax.broadcasted_iota(jnp.int32, (members, 8, cols), 1)
    rest_low = jnp.where(row == 6, over_slots(jnp.broadcast_to(rest_power, rest.shape)), over_slots(rest_low))
    decs_power = over_parts(jnp.broadcast_to(decs_power, decs.shape))
    rest_high = jnp.where(row == 6, weights_power, jnp.where(row == 7, decs_power, over_slots(rest_high)))
    full = jnp.concatenate([weights, over_parts(decs), rest_high, rest_low], axis=1)
    coded[...] = jnp.round(full).astype(jnp.int32).astype(jnp.int16)


def encode(mine, other, slots, parts):
    depth, cols = mine.shape[1:]
    vmem = pl.BlockSpec(memory_space=pltpu.VMEM)
    return pl.pallas_call(
        functools.partial(encode_kernel, slots, parts),
        name="encode",
        out_shape=jax.ShapeDtypeStruct((slots * parts, depth + 24, cols), jnp.int16),
        in_specs=[vmem, vmem],
        out_specs=vmem,
        compiler_params=pltpu.CompilerParams(vmem_limit_bytes=16 * 1024 * 1024),
    )(mine, other)


def sum_kernel(scale, parts, spread, rest):
    depth = spread.shape[1] - 8
    weights = depth - 8
    cols = spread.shape[2]
    values = parts[...].astype(jnp.int32).astype(F32)
    high, low = values[:, depth : depth + 8], values[:, depth + 8 : depth + 16]

    def unit(row):
        return jnp.exp2(row - 14.0) * scale

    def scaled_part(part):
        peak = jnp.max(jnp.abs(part), axis=0, keepdims=True)
        power = jnp.floor(jnp.log2(jnp.maximum(peak, 1e-30))) + 1.0
        return part * jnp.exp2(14.0 - power), power

    main = jnp.sum(values[:, :weights] * unit(high[:, 6:7]), axis=0)
    decs = jnp.sum(values[:, weights:depth] * unit(high[:, 7:8]), axis=0)
    rest[...] = jnp.sum((high + low * (1.0 / 16384.0)) * unit(low[:, 6:7]), axis=0)
    main, main_power = scaled_part(main)
    decs, decs_power = scaled_part(decs)
    row = lax.broadcasted_iota(jnp.int32, (8, cols), 0)
    powers = jnp.where(row == 0, main_power, decs_power)
    full = jnp.round(jnp.concatenate([main, decs, powers], axis=0))
    full = full.astype(jnp.int32)[None]
    spread[...] = jnp.broadcast_to(full, spread.shape).astype(jnp.int16)


def sum_parts(parts, slots, scale):
    _, depth, cols = parts.shape
    vmem = pl.BlockSpec(memory_space=pltpu.VMEM)
    return pl.pallas_call(
        functools.partial(sum_kernel, scale),
        name="sum_parts",
        out_shape=(
            jax.ShapeDtypeStruct((slots, depth - 8, cols), jnp.int16),
            jax.ShapeDtypeStruct((8, cols), F32),
        ),
        in_specs=[vmem],
        out_specs=(vmem, vmem),
        compiler_params=pltpu.CompilerParams(vmem_limit_bytes=16 * 1024 * 1024),
    )(parts)


def lay_kernel(place, mine, other, w_in, w_out, dec):
    core = place[0]
    slots, depth, cols = mine.shape
    weights = depth - 16
    width = w_in.shape[0]
    deep = width // slots

    def decoded(part):
        values = part[...].astype(jnp.int32).astype(F32)
        units = jnp.exp2(values[:, weights + 8 :] - 14.0)
        return values[:, :weights] * units[:, 0:1], values[:, weights : weights + 8] * units[:, 1:2]

    def lay(low, high):
        low, low_dec = decoded(low)
        high, high_dec = decoded(high)
        for p in range(w_in.shape[1] // cols):
            rows = slice(p * deep, (p + 1) * deep)
            block = slice(p * cols, (p + 1) * cols)
            w_in[block, :] = jnp.transpose(low[:, rows, :].reshape(width, cols))
            w_out[:, block] = high[:, rows, :].reshape(width, cols)
        dec[: slots * 8, :] = low_dec.reshape(slots * 8, cols)
        dec[slots * 8 :, :] = high_dec.reshape(slots * 8, cols)

    pl.when(core == 0)(lambda: lay(mine, other))
    pl.when(core == 1)(lambda: lay(other, mine))


def lay_out(place, mine, other, width, share, cols):
    vmem = pl.BlockSpec(memory_space=pltpu.VMEM)
    shape = jax.ShapeDtypeStruct
    return pl.pallas_call(
        lay_kernel,
        name="lay_out",
        out_shape=(
            shape((width, share), F32),
            shape((share, width), F32),
            shape((width, cols), F32),
        ),
        in_specs=[pl.BlockSpec(memory_space=pltpu.SMEM), vmem, vmem],
        out_specs=(vmem,) * 3,
        compiler_params=pltpu.CompilerParams(vmem_limit_bytes=8 * 1024 * 1024),
    )(place, mine, other)


AXES = ("y", "z", "c", "x")
RING = ("x", "y", "z")


def shifted(array, axis, by):
    count = lax.axis_size(axis)
    return lax.ppermute(array, axis, [(i, (i + by) % count) for i in range(count)])


def on_device(
    init_state,
    brownian,
    step_size,
    lengths,
    obs_steps,
    observed,
    w_in,
    b_in,
    w_out,
    b_out,
    decoder,
    prior_rate,
    diffusion,
):
    width = init_state.shape[1]
    share = w_in.shape[1]
    parts = lax.axis_size("x")
    slots = lax.axis_size("y") * lax.axis_size("z")
    cols = decoder.shape[1]
    core = lax.axis_index("c")
    spot = lax.axis_index("x")

    tall = ((0, 16), (0, 0))
    row = lax.broadcasted_iota(jnp.int32, (width + 16, share), 0)
    own = jnp.where(core == 0, jnp.pad(w_in, tall), jnp.pad(w_out, tall))
    half = jnp.where(row < width, own, b_in[None])
    halves = [half] + [shifted(half, "x", by) for by in range(1, parts)]
    packed = jnp.concatenate([init_state, b_out[None], prior_rate[None], diffusion[None]], axis=0)
    vectors = jnp.concatenate(
        [step_size[None], lengths.astype(F32)[None], obs_steps.T.astype(F32)], axis=0
    )
    by_slot = jnp.transpose(observed, (1, 0, 2))
    _, w_in, w_out = lax.optimization_barrier((half, w_in, w_out))
    rest = jnp.where(core == 0, w_out, w_in)
    halves[1], packed, vectors, dec, by_slot, rest = lax.optimization_barrier(
        (halves[1], packed, vectors, decoder.astype(F32), by_slot, rest)
    )
    rests = [rest] + [shifted(got, "c", 1) for got in halves[1:]]
    place = jnp.stack([core, spot]).astype(jnp.int32)
    keep, send, elbo, grad_init = solve(
        (brownian, packed, vectors, dec, by_slot), halves, rests, place, slots
    )
    scale = 1.0 / (init_state.shape[0] * lax.axis_size(AXES))
    coded = encode(keep, shifted(send, "c", 1), slots, parts)
    received = lax.all_to_all(coded, RING, 0, 0, tiled=True)
    spread, rest = sum_parts(received, slots, scale)
    own = lax.all_to_all(spread, ("y", "z"), 0, 0, tiled=True)
    other = shifted(own, "c", 1)
    grad_w_in, grad_w_out, grad_decoder = lay_out(place, own, other, width, share, cols)
    per = share // cols
    end = per + width // cols
    return (
        elbo.reshape(-1),
        jnp.sum(rest[end : end + 2], axis=1),
        grad_w_in,
        rest[:per].reshape(-1),
        grad_w_out,
        rest[per:end].reshape(-1),
        grad_decoder,
        grad_init,
    )


def solution(mesh):
    torus = Mesh(mesh.devices.reshape(4, 4, 2, mesh.shape["mp"]), AXES)
    return jax.shard_map(
        on_device,
        mesh=torus,
        in_specs=(
            P(AXES, None),
            P(None, AXES, None),
            P(AXES),
            P(AXES),
            P(AXES, None),
            P(AXES, None, None),
            P(None, "x"),
            P("x"),
            P("x", None),
            P(),
            P(),
            P(),
            P(),
        ),
        out_specs=(
            P(AXES),
            P(),
            P(None, "x"),
            P("x"),
            P("x", None),
            P(),
            P(),
            P(AXES, None),
        ),
        check_vma=False,
    )
```

```python
import functools

import jax
import jax.numpy as jnp
from jax import lax
from jax.experimental import pallas as pl
from jax.experimental.pallas import tpu as pltpu
from jax.sharding import Mesh
from jax.sharding import PartitionSpec as P

F32 = jnp.float32
BF16 = jnp.bfloat16


def wide(x):
    return jnp.concatenate([x, x], axis=1)


def column(row, rows):
    return jnp.transpose(jnp.broadcast_to(row, (rows, rows)))


def series_kernel(
    brown_home,
    packed,
    vectors,
    dec_home,
    obs,
    half_0,
    half_1,
    half_2,
    half_3,
    rest_0,
    rest_1,
    rest_2,
    rest_3,
    place,
    keep,
    send,
    elbo,
    grad_init,
    act,
    seen_back,
    low,
    pg_a,
    pg_b,
    upd_a,
    upd_b,
    scaled,
    b_in,
    w_in,
    w_out,
    w_in_t,
    w_out_t,
    obs_at,
    state,
    kl_acc,
    sq_acc,
    in_acc,
    out_acc,
    acc,
    acc_dec,
    dec,
    seen_now,
    moved,
    before,
    brown,
    done,
):
    fetch = pltpu.make_async_copy(brown_home, brown, done)
    fetch.start()
    steps, rows, width = brown.shape
    halves = (half_0, half_1, half_2, half_3)
    rests = (rest_0, rest_1, rest_2, rest_3)
    parts = len(halves)
    share = half_0.shape[1]
    hidden = parts * share
    cols = dec.shape[1]
    seen = obs.shape[0]
    first, last_row = packed[:rows, :], packed[rows : rows + 3, :]
    b_out, prior, diff = last_row[0:1], last_row[1:2], last_row[2:3]
    step, lens = vectors[0:1, :], vectors[1:2, :]
    dec[...] = dec_home[...].astype(BF16)

    core = place[0]

    def unpack(ins, outs):
        for q in range(parts):
            block = slice(q * share, (q + 1) * share)
            w_in[q] = ins[q][:width, :]
            w_out[block, :] = outs[q][:width, :]
            w_in_t[block, :] = jnp.transpose(ins[q][:width, :])
            w_out_t[q] = jnp.transpose(outs[q][:width, :])

    pl.when(core == 0)(lambda: unpack(halves, rests))
    pl.when(core == 1)(lambda: unpack(rests, halves))
    for q in range(parts):
        b_in[:, q * share : (q + 1) * share] = halves[q][width:, :].astype(F32)[:1]

    step_b = column(step, rows)
    root_b = jnp.sqrt(step_b)
    lens_b = column(lens, rows)
    inv = 1.0 / diff
    for j in range(seen):
        obs_at[j] = column(vectors[2 + j : 3 + j, :], rows)
    dec_t = jnp.transpose(dec[...])
    w_in_t[hidden : hidden + cols, :] = dec_t
    w_in_t[hidden + cols : hidden + 2 * cols, :] = dec_t

    state[...] = first
    kl_acc[...] = jnp.zeros_like(kl_acc)
    sq_acc[...] = jnp.zeros_like(sq_acc)
    in_acc[...] = jnp.zeros_like(in_acc)
    out_acc[...] = jnp.zeros_like(out_acc)
    acc[...] = jnp.zeros_like(acc)
    acc_dec[...] = jnp.zeros_like(acc_dec)

    early = 4
    seen_now[...] = jnp.zeros_like(seen_now)
    moved[...] = jnp.broadcast_to(-b_out, (rows, width))
    before[...] = jnp.zeros_like(before)

    def observe_some(k, which, total, squares):
        stamp = k.astype(F32)
        product = seen_now[...]
        for j in which:
            misfit = jnp.where(obs_at[j] == stamp, product - obs[j].astype(F32), 0.0)
            squares = squares + misfit * misfit
            total = total + misfit.astype(BF16).astype(F32)
        return total, squares

    def store_back(total, at):
        high = total.astype(BF16)
        seen_back[at, :, :cols] = high
        seen_back[at, :, cols:] = (total - high.astype(F32)).astype(BF16)

    def observe(k, at):
        total, squares = observe_some(k, range(seen), jnp.zeros((rows, cols), F32), sq_acc[...])
        sq_acc[...] = squares
        store_back(total, at)

    def settle(k):
        at = jnp.maximum(k, 0)
        factor = wide(jnp.where(k.astype(F32) < lens_b, step_b, 0.0))
        residual = (moved[...] + b_out + prior * before[...]) * inv
        scaled[at] = residual * inv
        spent = factor * (residual * residual)
        kl_acc[...] += spent[:, :rows] + spent[:, rows:]

    def forward(k, _):
        now = state[...]
        low_now = now.astype(BF16)
        low[k] = low_now
        live = k.astype(F32) < lens_b
        factor = wide(jnp.where(live, step_b, 0.0))
        noise = wide(jnp.where(live, root_b, 0.0))
        base = now + (factor * b_out + diff * noise * brown[k].astype(F32))
        past = k - 1
        total, squares = observe_some(
            past, range(early), jnp.zeros((rows, cols), F32), sq_acc[...]
        )
        floor = jnp.min((squares + jnp.abs(total)).reshape(rows // 8, 8, cols), axis=0)
        nothing = wide(jnp.minimum(floor, 0.0))[None]
        for q in range(parts):
            block = slice(q * share, (q + 1) * share)
            pre = jnp.dot(low_now, w_in[q], preferred_element_type=F32)
            if q == 0:
                pre = (pre.reshape(rows // 8, 8, share) + (nothing + b_in[:, block])).reshape(
                    rows, share
                )
            else:
                pre = pre + b_in[:, block]
            act[k, :, block] = jnp.tanh(pre).astype(BF16)
        settle(past)
        total, squares = observe_some(past, range(early, seen), total, squares)
        sq_acc[...] = squares
        store_back(total, jnp.maximum(past, 0))
        seen_now[...] = jnp.dot(low_now, dec[...], preferred_element_type=F32)
        product = jnp.dot(act[k], w_out[...], preferred_element_type=F32)
        moved[...] = product
        before[...] = now
        state[...] = base + factor * product
        return 0

    fetch.wait()
    lax.fori_loop(0, steps, forward, 0)
    settle(jnp.int32(steps - 1))
    observe(jnp.int32(steps - 1), steps - 1)
    last = state[...].astype(BF16)
    low[steps] = last
    seen_now[...] = jnp.dot(last, dec[...], preferred_element_type=F32)
    observe(jnp.int32(steps), steps)

    state[...] = jnp.dot(
        seen_back[steps], w_in_t[hidden:, :], preferred_element_type=F32
    )

    turned = (((0,), (0,)), ((), ()))

    def back_pair(k_low, pg_now, upd_now):
        for slot in (1, 0):
            k = k_low + slot
            cot = state[...]
            factor = wide(jnp.where(k.astype(F32) < lens_b, step_b, 0.0))
            pull = scaled[k]
            update = factor * (cot + pull)
            low_up = update.astype(BF16)
            upd_now[slot] = low_up
            out_acc[...] += jnp.sum(update.reshape(rows // 8, 8, width), axis=0)
            for q in range(parts):
                block = slice(q * share, (q + 1) * share)
                a = act[k, :, block].astype(F32)
                pre = jnp.dot(low_up, w_out_t[q], preferred_element_type=F32) * (1.0 - a * a)
                pg_now[slot, :, block] = pre.astype(BF16)
                in_acc[:, block] += jnp.sum(pre.reshape(rows // 8, 8, share), axis=0)
            pg_now[slot, :, hidden:] = seen_back[k]
            state[...] = (
                cot
                + factor * (prior * pull)
                + jnp.dot(pg_now[slot], w_in_t[...], preferred_element_type=F32)
            )

    def add_grads(k_low, pg_then, upd_then):
        at = pl.ds(k_low, 2)
        right = low[at].reshape(2 * rows, width)
        left = pg_then[...].reshape(2 * rows, hidden + 2 * cols)
        acc[0] += lax.dot_general(left[:, :hidden], right, turned, preferred_element_type=F32)
        acc_dec[...] += lax.dot_general(
            left[:, hidden:], right, turned, preferred_element_type=F32
        )
        acc[1] += lax.dot_general(
            act[at].reshape(2 * rows, hidden),
            upd_then[...].reshape(2 * rows, width),
            turned,
            preferred_element_type=F32,
        )

    pg_b[...] = jnp.zeros_like(pg_b)
    upd_b[...] = jnp.zeros_like(upd_b)

    def backward(i, _):
        k = steps - 4 - 4 * i
        back_pair(k + 2, pg_a, upd_a)
        add_grads(jnp.minimum(k + 4, steps - 2), pg_b, upd_b)
        back_pair(k, pg_b, upd_b)
        add_grads(k + 2, pg_a, upd_a)
        return 0

    lax.fori_loop(0, steps // 4, backward, 0, unroll=4)
    add_grads(0, pg_b, upd_b)
    grad_init[...] = state[...]
    final = acc_dec[...] + lax.dot_general(
        seen_back[steps], low[steps], turned, preferred_element_type=F32
    )
    spot = place[1]
    lanes = share // cols
    blocks, depth, _ = keep.shape
    slots = width * lanes // depth
    deep = width // slots
    members = slots * parts
    tile = slots * 8
    acc_dec[:, :cols] = jnp.transpose(final[:cols, :] + final[cols:, :])
    in_sum = jnp.sum(in_acc[...], axis=0, keepdims=True)
    out_sum = jnp.sum(out_acc[...], axis=0, keepdims=True)
    kl = 0.5 * jnp.sum(jnp.transpose(kl_acc[...]), axis=0, keepdims=True)
    loglik = -0.5 * jnp.sum(jnp.transpose(sq_acc[...]), axis=0, keepdims=True)
    rest = [out_sum[:, p * cols : (p + 1) * cols] for p in range(width // cols)]
    rest = rest + [loglik, kl]
    rest = rest + [jnp.zeros((8 - lanes - len(rest), cols), F32)]
    for half, out in ((core, keep), (1 - core, send)):
        decs = acc_dec[pl.ds(pl.multiple_of(half * tile, 8), tile), :cols]
        out[members : members + tile // depth] = decs.reshape(tile // depth, depth, cols)
        for s in range(parts):
            q = lax.rem(spot + (parts - s), parts)
            at = pl.ds(q * slots, slots)
            for p in range(lanes):
                block = slice(s * share, (s + 1) * share)
                out[at, p * deep : (p + 1) * deep, :] = acc[
                    half, block, p * cols : (p + 1) * cols
                ].reshape(slots, deep, cols)
            aux = [in_sum[:, s * share + p * cols : s * share + (p + 1) * cols] for p in range(lanes)]
            out[blocks - 1, pl.ds(pl.multiple_of(q * 8, 8), 8), :] = jnp.concatenate(
                aux + rest, axis=0
            )

    divisor = width * lens + cols * seen
    elbo[...] = (loglik - kl) / divisor


def solve(operands, halves, rests, place, slots):
    brown, packed, vectors, dec, observed = operands
    rows, width = brown.shape[1:]
    steps = brown.shape[0]
    parts = len(halves)
    share = halves[0].shape[1]
    hidden = parts * share
    seen, _, cols = observed.shape
    vmem = pl.BlockSpec(memory_space=pltpu.VMEM)
    shape = jax.ShapeDtypeStruct
    depth = width // slots * share // cols
    payload = shape((slots * parts + slots * 8 // depth + parts * 8 // depth, depth, cols), F32)
    outs = (
        payload,
        payload,
        shape((1, rows), F32),
        shape((rows, width), F32),
    )
    return pl.pallas_call(
        series_kernel,
        name="series",
        out_shape=outs,
        in_specs=[pl.BlockSpec(memory_space=pltpu.HBM)]
        + [vmem] * (4 + 2 * parts)
        + [pl.BlockSpec(memory_space=pltpu.SMEM)],
        out_specs=(vmem,) * len(outs),
        scratch_shapes=[
            pltpu.VMEM((steps, rows, hidden), BF16),
            pltpu.VMEM((steps + 1, rows, 2 * cols), BF16),
            pltpu.VMEM((steps + 1, rows, width), BF16),
            pltpu.VMEM((2, rows, hidden + 2 * cols), BF16),
            pltpu.VMEM((2, rows, hidden + 2 * cols), BF16),
            pltpu.VMEM((2, rows, width), BF16),
            pltpu.VMEM((2, rows, width), BF16),
            pltpu.VMEM((steps, rows, width), F32),
            pltpu.VMEM((1, hidden), F32),
            pltpu.VMEM((parts, width, share), BF16),
            pltpu.VMEM((hidden, width), BF16),
            pltpu.VMEM((hidden + 2 * cols, width), BF16),
            pltpu.VMEM((parts, width, share), BF16),
            pltpu.VMEM((seen, rows, cols), F32),
            pltpu.VMEM((rows, width), F32),
            pltpu.VMEM((rows, rows), F32),
            pltpu.VMEM((rows, cols), F32),
            pltpu.VMEM((8, hidden), F32),
            pltpu.VMEM((8, width), F32),
            pltpu.VMEM((2, hidden, width), F32),
            pltpu.VMEM((2 * cols, width), F32),
            pltpu.VMEM((width, cols), BF16),
            pltpu.VMEM((rows, cols), F32),
            pltpu.VMEM((rows, width), F32),
            pltpu.VMEM((rows, width), F32),
            pltpu.VMEM((steps, rows, width), BF16),
            pltpu.SemaphoreType.DMA,
        ],
        compiler_params=pltpu.CompilerParams(
            vmem_limit_bytes=50 * 1024 * 1024,
        ),
        cost_estimate=pl.CostEstimate(
            flops=12 * steps * rows * width * hidden,
            bytes_accessed=8 * 1024 * 1024,
            transcendentals=steps * rows * hidden,
        ),
    )(
        *operands,
        *halves,
        *rests,
        place,
    )


def encode_kernel(slots, parts, mine, other, coded):
    depth, cols = mine.shape[1:]
    members = slots * parts
    decs_end = members + slots * 8 // depth
    total = mine[...] + other[...]

    def scaled_part(part):
        peak = jnp.max(jnp.abs(part), axis=1, keepdims=True)
        power = jnp.floor(jnp.log2(jnp.maximum(peak, 1e-30))) + 1.0
        return part * jnp.exp2(14.0 - power), power

    def over_slots(part):
        full = jnp.broadcast_to(part[:, None], (parts, slots, *part.shape[1:]))
        return full.reshape(members, *part.shape[1:])

    def over_parts(part):
        full = jnp.broadcast_to(part[None], (parts, *part.shape))
        return full.reshape(members, *part.shape[1:])

    weights, weights_power = scaled_part(total[:members])
    decs, decs_power = scaled_part(total[members:decs_end].reshape(slots, 8, cols))
    rest, rest_power = scaled_part(total[decs_end:].reshape(parts, 8, cols))
    rest_high = jnp.round(rest)
    rest_low = (rest - rest_high) * 16384.0
    row = lax.broadcasted_iota(jnp.int32, (members, 8, cols), 1)
    rest_low = jnp.where(row == 6, over_slots(jnp.broadcast_to(rest_power, rest.shape)), over_slots(rest_low))
    decs_power = over_parts(jnp.broadcast_to(decs_power, decs.shape))
    rest_high = jnp.where(row == 6, weights_power, jnp.where(row == 7, decs_power, over_slots(rest_high)))
    full = jnp.concatenate([weights, over_parts(decs), rest_high, rest_low], axis=1)
    coded[...] = jnp.round(full).astype(jnp.int32).astype(jnp.int16)


def encode(mine, other, slots, parts):
    depth, cols = mine.shape[1:]
    vmem = pl.BlockSpec(memory_space=pltpu.VMEM)
    return pl.pallas_call(
        functools.partial(encode_kernel, slots, parts),
        name="encode",
        out_shape=jax.ShapeDtypeStruct((slots * parts, depth + 24, cols), jnp.int16),
        in_specs=[vmem, vmem],
        out_specs=vmem,
        compiler_params=pltpu.CompilerParams(vmem_limit_bytes=16 * 1024 * 1024),
    )(mine, other)


def sum_kernel(scale, parts, spread, rest):
    depth = spread.shape[1] - 8
    weights = depth - 8
    cols = spread.shape[2]
    values = parts[...].astype(jnp.int32).astype(F32)
    high, low = values[:, depth : depth + 8], values[:, depth + 8 : depth + 16]

    def unit(row):
        return jnp.exp2(row - 14.0) * scale

    def scaled_part(part):
        peak = jnp.max(jnp.abs(part), axis=0, keepdims=True)
        power = jnp.floor(jnp.log2(jnp.maximum(peak, 1e-30))) + 1.0
        return part * jnp.exp2(14.0 - power), power

    main = jnp.sum(values[:, :weights] * unit(high[:, 6:7]), axis=0)
    decs = jnp.sum(values[:, weights:depth] * unit(high[:, 7:8]), axis=0)
    rest[...] = jnp.sum((high + low * (1.0 / 16384.0)) * unit(low[:, 6:7]), axis=0)
    main, main_power = scaled_part(main)
    decs, decs_power = scaled_part(decs)
    row = lax.broadcasted_iota(jnp.int32, (8, cols), 0)
    powers = jnp.where(row == 0, main_power, decs_power)
    full = jnp.round(jnp.concatenate([main, decs, powers], axis=0))
    full = full.astype(jnp.int32)[None]
    spread[...] = jnp.broadcast_to(full, spread.shape).astype(jnp.int16)


def sum_parts(parts, slots, scale):
    _, depth, cols = parts.shape
    vmem = pl.BlockSpec(memory_space=pltpu.VMEM)
    return pl.pallas_call(
        functools.partial(sum_kernel, scale),
        name="sum_parts",
        out_shape=(
            jax.ShapeDtypeStruct((slots, depth - 8, cols), jnp.int16),
            jax.ShapeDtypeStruct((8, cols), F32),
        ),
        in_specs=[vmem],
        out_specs=(vmem, vmem),
        compiler_params=pltpu.CompilerParams(vmem_limit_bytes=16 * 1024 * 1024),
    )(parts)


def lay_kernel(place, mine, other, rest, w_in, w_out, dec, b_in, b_out):
    core = place[0]
    slots, depth, cols = mine.shape
    weights = depth - 16
    width = w_in.shape[0]
    deep = width // slots

    def decoded(part):
        values = part[...].astype(jnp.int32).astype(F32)
        units = jnp.exp2(values[:, weights + 8 :] - 14.0)
        return values[:, :weights] * units[:, 0:1], values[:, weights : weights + 8] * units[:, 1:2]

    def lay(low, high):
        low, low_dec = decoded(low)
        high, high_dec = decoded(high)
        for p in range(w_in.shape[1] // cols):
            rows = slice(p * deep, (p + 1) * deep)
            block = slice(p * cols, (p + 1) * cols)
            w_in[block, :] = jnp.transpose(low[:, rows, :].reshape(width, cols))
            w_out[:, block] = high[:, rows, :].reshape(width, cols)
        dec[: slots * 8, :] = low_dec.reshape(slots * 8, cols)
        dec[slots * 8 :, :] = high_dec.reshape(slots * 8, cols)

    lanes = b_in.shape[1] // cols
    for p in range(lanes):
        b_in[:, p * cols : (p + 1) * cols] = rest[p : p + 1, :]
    for p in range(width // cols):
        b_out[:, p * cols : (p + 1) * cols] = rest[lanes + p : lanes + p + 1, :]
    pl.when(core == 0)(lambda: lay(mine, other))
    pl.when(core == 1)(lambda: lay(other, mine))


def lay_out(place, mine, other, rest, width, share, cols):
    vmem = pl.BlockSpec(memory_space=pltpu.VMEM)
    shape = jax.ShapeDtypeStruct
    return pl.pallas_call(
        lay_kernel,
        name="lay_out",
        out_shape=(
            shape((width, share), F32),
            shape((share, width), F32),
            shape((width, cols), F32),
            shape((1, share), F32),
            shape((1, width), F32),
        ),
        in_specs=[pl.BlockSpec(memory_space=pltpu.SMEM), vmem, vmem, vmem],
        out_specs=(vmem,) * 5,
        compiler_params=pltpu.CompilerParams(vmem_limit_bytes=8 * 1024 * 1024),
    )(place, mine, other, rest)


AXES = ("y", "z", "c", "x")
RING = ("x", "y", "z")


def shifted(array, axis, by):
    count = lax.axis_size(axis)
    return lax.ppermute(array, axis, [(i, (i + by) % count) for i in range(count)])


def on_device(
    init_state,
    brownian,
    step_size,
    lengths,
    obs_steps,
    observed,
    w_in,
    b_in,
    w_out,
    b_out,
    decoder,
    prior_rate,
    diffusion,
):
    width = init_state.shape[1]
    share = w_in.shape[1]
    parts = lax.axis_size("x")
    slots = lax.axis_size("y") * lax.axis_size("z")
    cols = decoder.shape[1]
    core = lax.axis_index("c")
    spot = lax.axis_index("x")

    tall = ((0, 16), (0, 0))
    row = lax.broadcasted_iota(jnp.int32, (width + 16, share), 0)
    own = jnp.where(core == 0, jnp.pad(w_in, tall), jnp.pad(w_out, tall))
    half = jnp.where(row < width, own, b_in[None])
    halves = [half] + [shifted(half, "x", by) for by in range(1, parts)]
    packed = jnp.concatenate([init_state, b_out[None], prior_rate[None], diffusion[None]], axis=0)
    vectors = jnp.concatenate(
        [step_size[None], lengths.astype(F32)[None], obs_steps.T.astype(F32)], axis=0
    )
    by_slot = jnp.transpose(observed, (1, 0, 2))
    _, w_in, w_out = lax.optimization_barrier((half, w_in, w_out))
    rest = jnp.where(core == 0, w_out, w_in)
    halves[1], packed, vectors, dec, by_slot, rest = lax.optimization_barrier(
        (halves[1], packed, vectors, decoder.astype(F32), by_slot, rest)
    )
    rests = [rest] + [shifted(got, "c", 1) for got in halves[1:]]
    place = jnp.stack([core, spot]).astype(jnp.int32)
    keep, send, elbo, grad_init = solve(
        (brownian, packed, vectors, dec, by_slot), halves, rests, place, slots
    )
    scale = 1.0 / (init_state.shape[0] * lax.axis_size(AXES))
    coded = encode(keep, shifted(send, "c", 1), slots, parts)
    received = lax.all_to_all(coded, RING, 0, 0, tiled=True)
    spread, rest = sum_parts(received, slots, scale)
    own = lax.all_to_all(spread, ("y", "z"), 0, 0, tiled=True)
    other = shifted(own, "c", 1)
    grad_w_in, grad_w_out, grad_decoder, grad_b_in, grad_b_out = lay_out(
        place, own, other, rest, width, share, cols
    )
    per = share // cols
    end = per + width // cols
    return (
        elbo.reshape(-1),
        jnp.sum(rest[end : end + 2], axis=1),
        grad_w_in,
        grad_b_in.reshape(-1),
        grad_w_out,
        grad_b_out.reshape(-1),
        grad_decoder,
        grad_init,
    )


def solution(mesh):
    torus = Mesh(mesh.devices.reshape(4, 4, 2, mesh.shape["mp"]), AXES)
    return jax.shard_map(
        on_device,
        mesh=torus,
        in_specs=(
            P(AXES, None),
            P(None, AXES, None),
            P(AXES),
            P(AXES),
            P(AXES, None),
            P(AXES, None, None),
            P(None, "x"),
            P("x"),
            P("x", None),
            P(),
            P(),
            P(),
            P(),
        ),
        out_specs=(
            P(AXES),
            P(),
            P(None, "x"),
            P("x"),
            P("x", None),
            P(),
            P(),
            P(AXES, None),
        ),
        check_vma=False,
    )
```
